256 devices in a mesh: gx: 16 (over x_hi, y, core), gy: 16 (over x_lo, z).
Axes of the slice: x: 4 (x_hi: 2, x_lo: 2; x = x_hi * 2 + x_lo), y: 4, z: 8, core: 2. Of those that a mesh axis runs over, the one named last changes fastest.
Arguments:
- u_old: float32 [3, 512, 512, 256], P(None, 'gx', 'gy'), may hold values from -0.6 to 0.6
- density: float32 [512, 512, 256], P('gx', 'gy'), may hold values from 0.5 to 2
- offsets: float32 [3, 4096, 128], P(None, ('gx', 'gy')), may hold values from 0 to 1
- forces: float32 [3, 4096, 128], P(None, ('gx', 'gy')), may hold values from -60 to 60
- base_x: int32 [4096, 128], P(('gx', 'gy')), may hold values from 0 to 31
- base_y: int32 [4096, 128], P(('gx', 'gy')), may hold values from 0 to 31
- base_z: int32 [4096, 128], P(('gx', 'gy')), may hold values from 0 to 255
- tile_count: int32 [256], P(('gx', 'gy')), may hold values from 1 to 16, as said below
Outputs:
- u_new: float32 [3, 512, 512, 256], P(None, 'gx', 'gy')
- marker_velocity: float32 [3, 4096, 128], P(None, ('gx', 'gy'))
The draws below stay inside these ranges and needn't reach their ends.
Inputs may be any that keep to these rules, and one draw needn't show every extreme that they name: `tile_count`: every draw has a device with exactly 16 live tiles; loads are skewed, with a mean near a quarter of that.
All inputs are finite; a program needn't handle non-finite values.
Results may differ from the reference program's by a relative error of at most 0.000075.
Values sent between devices are 32-bit elements; how exact they have to be, the bound alone decides.
A program may use at most 64 MiB of HBM per device.

```python
import math
import jax
import jax.numpy as jnp

CX = 32
CY = 32
NZ = 256
TILE = 128
MAXT = 16
NX = 512
NY = 512
TILES = 4096
N_GY = 16
DEVICES = 256


def draw_tile_count(key, part):
    first, second, third = jax.random.split(jax.random.fold_in(key, 17), 3)
    upper = jax.random.randint(first, (DEVICES,), 0, MAXT)
    lower = jax.random.randint(second, (DEVICES,), 0, MAXT)
    counts = 1 + upper * lower // MAXT
    busiest = jax.random.randint(third, (), 0, DEVICES)
    return jnp.where(jnp.arange(DEVICES) == busiest, MAXT, counts).astype(jnp.int32)


def plant(drawn, key, least, top_value):
    index_at = [jax.random.randint(jax.random.fold_in(key, axis), (), 0, length) for axis, length in enumerate(drawn.shape)]
    widest = drawn.shape.index(max(drawn.shape))
    next_to = index_at[:widest] + [(index_at[widest] + 1) % drawn.shape[widest]] + index_at[widest + 1:]
    return drawn.at[tuple(index_at)].set(least).at[tuple(next_to)].set(top_value)


def block_levels(stream_key, dims, shards, least, largest):
    level, own = 1.0, jax.random.fold_in(stream_key, 6)
    for dim, shards_of in shards:
        steps = jnp.exp(jax.random.uniform(jax.random.fold_in(own, dim), (shards_of,), jnp.float32, least / len(shards), largest / len(shards)))
        level = level * jnp.repeat(steps, dims[dim] // shards_of).reshape([-1 if axis == dim else 1 for axis in range(len(dims))])
    return level


def noise(own_key, dims, scale, most, cuts=(), kind=jnp.bfloat16):
    drawn = jax.random.normal(own_key, dims, jnp.float32) * scale
    if len(cuts) > 0:
        drawn = block_levels(own_key, dims, cuts, -0.22, 0.18) * drawn
    return jnp.clip(drawn, min=-most, max=most).astype(kind)


def setup_inputs(seed: int = 0) -> dict:
    key_list = jax.random.split(jax.random.key(seed), 9)
    return {
        "u_old": noise(key_list[0], (3, NX, NY, NZ), 0.1, 0.6, ((1, 16), (2, 16)), jnp.float32),
        "density": jnp.clip(jnp.exp(math.log(2.0) - 1.3862944 * jax.random.uniform(key_list[1], (NX, NY, NZ), jnp.float32) ** block_levels(key_list[1], (NX, NY, NZ), ((0, 16), (1, 16)), -0.2, 0.2)), 0.5, 2.0),
        "offsets": jnp.clip(1.0 * jax.random.uniform(key_list[2], (3, TILES, TILE), jnp.float32) ** block_levels(key_list[2], (3, TILES, TILE), ((1, 256),), -0.2, 0.2), 0.0, 1.0),
        "forces": noise(key_list[3], (3, TILES, TILE), 10.0, 60.0, ((1, 256),), jnp.float32),
        "base_x": plant(jax.random.randint(key_list[4], (TILES, TILE), 0, CX), jax.random.fold_in(key_list[4], 1), 0, CX - 1).astype(jnp.int32),
        "base_y": plant(jax.random.randint(key_list[5], (TILES, TILE), 0, CY), jax.random.fold_in(key_list[5], 1), 0, CY - 1).astype(jnp.int32),
        "base_z": plant(jax.random.randint(key_list[6], (TILES, TILE), 0, NZ), jax.random.fold_in(key_list[6], 1), 0, NZ - 1).astype(jnp.int32),
        "tile_count": draw_tile_count(jax.random.fold_in(key_list[8], 71), 0),
    }


def stencil(frac):
    root = jnp.sqrt(1.0 + 4.0 * frac - 4.0 * frac * frac)
    return [(3.0 - 2.0 * frac - root) / 8.0, (3.0 - 2.0 * frac + root) / 8.0, (1.0 + 2.0 * frac + root) / 8.0, (1.0 + 2.0 * frac - root) / 8.0]

def reference(u_old, density, offsets, forces, base_x, base_y, base_z, tile_count):
    time_step = 0.5
    tiles, width = base_x.shape
    nx, ny, nz = density.shape
    slot = jnp.arange(tiles).astype(jnp.int32)
    device = slot // MAXT
    anchor_x = (device // N_GY * CX)[:, None]
    anchor_y = (device % N_GY * CY)[:, None]
    live = (slot % MAXT < tile_count[device]).astype(jnp.float32)[:, None] * jnp.ones((tiles, width), jnp.float32)
    weight_x = stencil(offsets[0])
    weight_y = stencil(offsets[1])
    weight_z = stencil(offsets[2])
    load = forces * live[None]
    grid = jnp.zeros((3, nx * ny * nz), jnp.float32)
    places = []
    for shift_a in range(4):
        cell_x = (anchor_x + base_x + shift_a - 1) % nx
        for shift_b in range(4):
            cell_y = (anchor_y + base_y + shift_b - 1) % ny
            for shift_c in range(4):
                cell_z = (base_z + shift_c - 1) % nz
                index = ((cell_x * ny + cell_y) * nz + cell_z).astype(jnp.int32)
                weight = weight_x[shift_a] * weight_y[shift_b] * weight_z[shift_c]
                grid = grid.at[:, index.reshape(-1)].add((load * weight[None]).reshape(3, -1))
                places.append((index, weight))
    force_grid = grid.reshape(3, nx, ny, nz)
    u_new = u_old + time_step * force_grid / density[None]
    table = u_new.reshape(3, -1)
    velocity = jnp.zeros((3, tiles, width), jnp.float32)
    for index, weight in places:
        velocity = velocity + table[:, index.reshape(-1)].reshape(3, tiles, width) * weight[None]
    return (u_new, velocity * live[None])
```

```python
import functools

import jax
import jax.numpy as jnp
from jax import lax
from jax.experimental import pallas as pl
from jax.experimental.pallas import tpu as pltpu
from jax.sharding import PartitionSpec as P

F32 = jnp.float32
I32 = jnp.int32
HBM = pltpu.HBM
VMEM = pltpu.VMEM
SMEM = pltpu.SMEM

SLOTS = 16
LANES = 128
SIDE = 32
NZ = 256
NT = 7
ZS, ZW = 37, 40
CS = 42
PLANES = 35
BLOCK = 40
STEP = NT * BLOCK
FRONT = 8
ROWS = 9856
COPIES = 4


def iota(shape, dim):
    return lax.broadcasted_iota(I32, shape, dim)


def four_weights(frac, root):
    low, high = 3.0 - 2.0 * frac, 1.0 + 2.0 * frac
    return [(low - root) * 0.125, (low + root) * 0.125, (high + root) * 0.125, (high - root) * 0.125]


def root_of(frac):
    return jnp.sqrt(1.0 + 4.0 * frac - 4.0 * frac * frac)


def row_index(bx, by, bz):
    z_tile = lax.shift_right_logical(bz * 1772, 16)
    return (bx * NT + z_tile) * BLOCK + by + FRONT


def columns_of(rows):
    rows = rows + [rows[-1]] * (-len(rows) % 8)
    return jnp.concatenate(rows, axis=0).T


def depth_weights(place, frac, root):
    away = iota((8, LANES), 1).astype(F32) - place
    away = jnp.where(away < 0.0, away + 128.0, away)
    first, second = away < CS - 0.5, away < 2 * CS - 0.5
    k = away - jnp.where(first, 0.0, jnp.where(second, float(CS), float(2 * CS)))
    value = jnp.where(k < 1.5, 3.0 - 2.0 * frac, 1.0 + 2.0 * frac)
    value = (value + jnp.where(jnp.abs(k - 1.5) < 1.0, root, -root)) * 0.125
    value = jnp.where(k < 3.5, value, 0.0)
    later = jnp.where(first, 0.0, value)
    return [jnp.where(first, value, 0.0), jnp.where(second, later, 0.0), jnp.where(second, 0.0, later)]


def z_place(bz):
    return lax.bitwise_and(bz + 127, 127).astype(F32)


def segments(t):
    found = []
    for half in range(2):
        for turn in (-1, 0, 1):
            low = max(ZS * t - 1 + NZ * turn - LANES * half, 0)
            high = min(ZS * t - 1 + ZW + NZ * turn - LANES * half, LANES)
            if low < high:
                found.append((half, low, high))
    return found


def lane_mask(c, low, high):
    lane = lax.bitwise_and(iota((8, LANES), 1) + (LANES - CS * c), 127)
    if low == 0:
        return lane < high
    if high == LANES:
        return lane >= low
    return jnp.logical_and(lane >= low, lane < high)


def spread_build(tile, count, offsets, forces, base_z, line, across):
    tile = jnp.minimum(tile, SLOTS - 1)
    live = jnp.where(tile < count, 1.0, 0.0)
    sx, sy, sz = (offsets[i, pl.ds(tile, 1), :] for i in range(3))
    push = [forces[c, pl.ds(tile, 1), :] * live for c in range(3)]
    table = columns_of(
        [z_place(base_z[pl.ds(tile, 1), :]), sz, root_of(sz)] + push + [sy, root_of(sy), sx, root_of(sx)]
    )
    for g in range(LANES // 8):
        wide = [jnp.broadcast_to(table[8 * g : 8 * g + 8, n : n + 1], (8, LANES)) for n in range(10)]
        depth = sum(w * part for w, part in zip(wide[3:6], depth_weights(*wide[:3])))
        for b, weight in enumerate(four_weights(wide[6], wide[7])):
            line[pl.ds(g * 32 + b, 8, stride=4), :] = weight * depth
        for a, weight in enumerate(four_weights(wide[8], wide[9])):
            across[a, 8 * g : 8 * g + 8, :] = weight


def spread_markers(tile, zero, index_s, line, across, grids):
    for first in range(0, LANES, COPIES):
        made = []
        for m in range(first, first + COPIES):
            start = index_s[tile, m]
            grid = grids[m - first]
            rows = line[pl.ds(zero + m * 4, 4), :]
            for a in range(4):
                where = pl.ds(start + a * STEP, 4)
                weight = jnp.broadcast_to(across[a, m : m + 1, :], (4, LANES))
                made.append((grid, where, grid[where, :] + weight * rows))
        for grid, where, value in made:
            grid[where, :] = value


def spread_kernel(
    count, offsets, forces, base_x, base_y, base_z, u_old, density,
    grid_out, strip_out, low_out, high_out,
    *scratch,
):
    grids = scratch[:COPIES]
    (index_v, index_s, line_a, line_b, across_a, across_b, planes, strips, edge_low, edge_high, low_v, high_v,
     sems, plane_sems) = scratch[COPIES:]
    index_v[...] = row_index(base_x[...], base_y[...], base_z[...])
    to_smem = pltpu.make_async_copy(index_v, index_s, sems.at[0])
    to_smem.start()
    edges = []
    for n, (first, place) in enumerate(((0, edge_low), (SIDE - 8, edge_high))):
        edges.append(pltpu.make_async_copy(u_old.at[:, :, pl.ds(first, 8), :], place.at[pl.ds(0, 3)], sems.at[1 + 2 * n]))
        edges.append(pltpu.make_async_copy(density.at[:, pl.ds(first, 8), :], place.at[3], sems.at[2 + 2 * n]))
    for copy in edges:
        copy.start()

    live_tiles = count[0]
    build = functools.partial(spread_build, count=live_tiles, offsets=offsets, forces=forces, base_z=base_z)
    build(jnp.int32(0), line=line_a, across=across_a)
    nothing = jnp.zeros((8, LANES), F32)

    @pl.loop(0, ROWS // 64)
    def _(i):
        for grid in grids:
            for j in range(8):
                grid[pl.ds(i * 64 + j * 8, 8), :] = nothing

    to_smem.wait()

    @pl.loop(0, lax.shift_right_logical(live_tiles + 1, 1))
    def _(turn):
        zero = jnp.minimum(turn, 0)
        build(2 * turn + 1, line=line_b, across=across_b)
        spread_markers(2 * turn, zero, index_s, line_a, across_a, grids)
        build(2 * turn + 2, line=line_a, across=across_a)
        spread_markers(2 * turn + 1, zero, index_s, line_b, across_b, grids)

    for copy in edges:
        copy.wait()
    row = iota((8, LANES), 0)
    last_row = row == 7
    three_rows = row < 3

    @pl.loop(0, SIDE)
    def _(x):
        for half in range(2):
            lanes = slice(half * LANES, (half + 1) * LANES)
            for c in range(4):
                low_v[half, pl.ds((x * 4 + c) * 2, 8), :] = edge_low[c, x, :, lanes]
                high_v[half, pl.ds(x * 4 + c, 8), :] = pltpu.roll(edge_high[c, x, :, lanes], 1, 0)

    def plane_copy(x):
        return pltpu.make_async_copy(planes.at[pl.ds(x, 1)], grid_out.at[pl.ds(x, 1)], plane_sems.at[x])

    @pl.loop(0, PLANES)
    def _(x):
        natural = []
        for yb in range(5):
            tiles = []
            for t in range(NT):
                start = FRONT + (x * NT + t) * BLOCK
                tile = sum(grid[pl.ds(start + 8 * yb + 1, 8), :] for grid in grids)
                if yb == 4:
                    tile = jnp.where(last_row, sum(grid[pl.ds(start - 7, 8), :] for grid in grids), tile)
                tiles.append(tile)
            sums = [[None, None] for _ in range(3)]
            for c in range(3):
                for half in range(2):
                    total = None
                    for group in ((0, 2, 4), (1, 3, 5), (6,)):
                        part = None
                        for t in group:
                            for at, low, high in segments(t):
                                if at == half:
                                    part = jnp.where(lane_mask(c, low, high), tiles[t], 0.0 if part is None else part)
                        if part is not None:
                            total = part if total is None else total + part
                    sums[c][half] = pltpu.roll(total, LANES - CS * c, 1) if c else total
            natural.append(sums)
        for c in range(3):
            for half in range(2):
                lanes = slice(half * LANES, (half + 1) * LANES)
                for yb in range(5):
                    planes[x, c, 8 * yb : 8 * yb + 8, lanes] = natural[yb][c][half]
                bottom, top, outside = (natural[yb][c][half] for yb in (0, 3, 4))
                where = pl.ds((x * 3 + c) * 3, 8)
                for side, value in enumerate((jnp.where(last_row, outside, bottom), jnp.where(last_row, top, outside))):
                    strips[side, half, where, :] = jnp.where(three_rows, pltpu.roll(value, 1, 0), 0.0)
        plane_copy(x).start()

    tail = [
        pltpu.make_async_copy(strips, strip_out, sems.at[0]),
        pltpu.make_async_copy(low_v, low_out, sems.at[1]),
        pltpu.make_async_copy(high_v, high_out, sems.at[2]),
    ]
    for copy in tail:
        copy.start()
    for copy in tail:
        copy.wait()

    @pl.loop(0, PLANES)
    def _(x):
        plane_copy(x).wait()


LOW_ROWS = 264
HIGH_ROWS = 136
YROWS = 320


def spread(count, offsets, forces, base_x, base_y, base_z, u_old, density):
    return pl.pallas_call(
        spread_kernel,
        name="spread",
        in_specs=[pl.BlockSpec(memory_space=SMEM)] + [pl.BlockSpec(memory_space=VMEM)] * 5 + [pl.BlockSpec(memory_space=HBM)] * 2,
        out_specs=[pl.BlockSpec(memory_space=HBM)] * 4,
        out_shape=[
            jax.ShapeDtypeStruct((PLANES, 3, 40, NZ), F32),
            jax.ShapeDtypeStruct((2, 2, YROWS, LANES), F32),
            jax.ShapeDtypeStruct((2, LOW_ROWS, LANES), F32),
            jax.ShapeDtypeStruct((2, HIGH_ROWS, LANES), F32),
        ],
        scratch_shapes=[VMEM((ROWS, LANES), F32)] * COPIES
        + [VMEM((SLOTS, LANES), I32), SMEM((SLOTS, LANES), I32)]
        + [VMEM((4 * LANES, LANES), F32)] * 2
        + [VMEM((4, LANES, LANES), F32)] * 2
        + [
            VMEM((PLANES, 3, 40, NZ), F32),
            VMEM((2, 2, YROWS, LANES), F32),
            VMEM((4, SIDE, 8, NZ), F32),
            VMEM((4, SIDE, 8, NZ), F32),
            VMEM((2, LOW_ROWS, LANES), F32),
            VMEM((2, HIGH_ROWS, LANES), F32),
            pltpu.SemaphoreType.DMA((5,)),
            pltpu.SemaphoreType.DMA((PLANES,)),
        ],
        compiler_params=pltpu.CompilerParams(vmem_limit_bytes=63 * 2**20),
    )(count, offsets, forces, base_x, base_y, base_z, u_old, density)


def exchange_kernel(
    grid, strip, low, high, u_old, density,
    rx, ry, rd, rlow, rhigh, ux_low, ux_high, dx_low, dx_high,
    send_sems, recv_sems,
):
    nx, ny = lax.axis_size("gx"), lax.axis_size("gy")
    gx, gy = lax.axis_index("gx"), lax.axis_index("gy")
    left, right = lax.rem(gx + nx - 1, nx), lax.rem(gx + 1, nx)
    down, up = lax.rem(gy + ny - 1, ny), lax.rem(gy + 1, ny)
    around = [(i, j) for i in (left, gx, right) for j in (down, gy, up)]
    del around[4]
    barrier = pltpu.get_barrier_semaphore()
    for place in around:
        pl.semaphore_signal(barrier, inc=1, device_id=place, device_id_type=pl.DeviceIdType.MESH)
    pl.semaphore_wait(barrier, len(around))
    last = pl.ds(SIDE - 1, 1)
    first = pl.ds(0, 2)
    rows = lambda start, size: pl.ds(start, size)
    moves = [
        (strip.at[1, :, rows(0, 320), :], ry.at[0], (gx, up)),
        (strip.at[0, :, rows(0, 320), :], ry.at[1], (gx, down)),
        (low.at[:, rows(0, 256), :], rlow.at[:, rows(8, 256), :], (gx, down)),
        (high.at[:, rows(0, 128), :], rhigh.at[:, rows(16, 128), :], (gx, up)),
        (grid.at[rows(SIDE, 3)], rx.at[0], (right, gy)),
        (grid.at[rows(0, 3)], rx.at[1], (left, gy)),
        (u_old.at[:, last], ux_low, (right, gy)),
        (u_old.at[:, first], ux_high, (left, gy)),
        (density.at[last], dx_low, (right, gy)),
        (density.at[first], dx_high, (left, gy)),
        (strip.at[1, :, rows(288, 32), :], rd.at[0], (right, up)),
        (high.at[:, rows(120, 8), :], rhigh.at[:, rows(8, 8), :], (right, up)),
        (strip.at[1, :, rows(0, 32), :], rd.at[1], (left, up)),
        (high.at[:, rows(0, 8), :], rhigh.at[:, rows(144, 8), :], (left, up)),
        (strip.at[0, :, rows(288, 32), :], rd.at[2], (right, down)),
        (low.at[:, rows(248, 8), :], rlow.at[:, rows(0, 8), :], (right, down)),
        (strip.at[0, :, rows(0, 32), :], rd.at[3], (left, down)),
        (low.at[:, rows(0, 16), :], rlow.at[:, rows(264, 16), :], (left, down)),
    ]
    copies = [
        pltpu.make_async_remote_copy(
            src_ref=source,
            dst_ref=target,
            send_sem=send_sems.at[n],
            recv_sem=recv_sems.at[n],
            device_id=place,
            device_id_type=pl.DeviceIdType.MESH,
        )
        for n, (source, target, place) in enumerate(moves)
    ]
    for copy in copies:
        copy.start()
    for copy in copies:
        copy.wait()


MOVES = 18
RLOW_ROWS, RHIGH_ROWS = 296, 160
EXCHANGED = (
    (2, 3, 3, 40, NZ),
    (2, 2, 320, LANES),
    (4, 2, 32, LANES),
    (2, RLOW_ROWS, LANES),
    (2, RHIGH_ROWS, LANES),
    (3, 1, SIDE, NZ),
    (3, 2, SIDE, NZ),
    (1, SIDE, NZ),
    (2, SIDE, NZ),
)


def exchange(grid, strip, low, high, u_old, density):
    return pl.pallas_call(
        exchange_kernel,
        name="exchange",
        in_specs=[pl.BlockSpec(memory_space=HBM)] * 6,
        out_specs=[pl.BlockSpec(memory_space=HBM)] * len(EXCHANGED),
        out_shape=[jax.ShapeDtypeStruct(shape, F32) for shape in EXCHANGED],
        scratch_shapes=[pltpu.SemaphoreType.DMA((MOVES,)), pltpu.SemaphoreType.DMA((MOVES,))],
        compiler_params=pltpu.CompilerParams(collective_id=0, has_side_effects=True),
    )(grid, strip, low, high, u_old, density)


def gather_build(tile, offsets, base_z, across, along, depth):
    tile = jnp.minimum(tile, SLOTS - 1)
    sx, sy, sz = (offsets[i, pl.ds(tile, 1), :] for i in range(3))
    table = columns_of([z_place(base_z[pl.ds(tile, 1), :]), sz, root_of(sz), sy, root_of(sy), sx, root_of(sx)])
    for g in range(LANES // 8):
        rows = slice(8 * g, 8 * g + 8)
        wide = [jnp.broadcast_to(table[rows, n : n + 1], (8, LANES)) for n in range(7)]
        for c, value in enumerate(depth_weights(wide[0], wide[1], wide[2])):
            depth[c, rows, :] = value
        for b, weight in enumerate(four_weights(wide[3], wide[4])):
            along[b, rows, :] = weight
        for a, weight in enumerate(four_weights(wide[5], wide[6])):
            across[a, rows, :] = weight


def gather_markers(tile, zero, count, index_s, table, across, along, depth, stage, velocity):
    for m in range(LANES):
        start = index_s[tile, m]
        total = None
        for a in range(4):
            term = jnp.broadcast_to(across[a, m : m + 1, :], (4, LANES)) * table[pl.ds(start + a * STEP, 4), :]
            total = term if total is None else total + term
        stage[pl.ds(zero + m * 4, 4), :] = total
    picked = [[] for _ in range(3)]
    for g in range(LANES // 8):
        rows = slice(8 * g, 8 * g + 8)
        total = None
        for b in range(4):
            term = along[b, rows, :] * stage[pl.ds(zero + g * 32 + b, 8, stride=4), :]
            total = term if total is None else total + term
        for c in range(3):
            picked[c].append(total * depth[c, rows, :])
    values = jnp.concatenate(picked[0] + picked[1] + picked[2], axis=0)
    rough = values.astype(jnp.bfloat16)
    rest = (values - rough.astype(F32)).astype(jnp.bfloat16)
    both = jnp.concatenate([rough, rest], axis=1)
    out = lax.dot_general(
        jnp.ones((8, 2 * LANES), jnp.bfloat16), both, (((1,), (1,)), ((), ())), preferred_element_type=F32
    )
    live = tile < count
    for c in range(3):
        velocity[c, pl.ds(tile, 1), :] = jnp.where(live, out[0:1, c * LANES : (c + 1) * LANES], 0.0)


def gather_kernel(
    count, offsets, base_x, base_y, base_z, u_old, density, grid,
    rx, ry, rd, rlow, rhigh, ux_low, ux_high, dx_low, dx_high,
    u_new, velocity,
    index_v, index_s, table, fluid, force, vx, vy, vd, vlow, vhigh,
    across_a, across_b, along_a, along_b, depth_a, depth_b, stage_a, stage_b, sems, plane_sems,
):
    index_v[...] = row_index(base_x[...], base_y[...], base_z[...])
    inner = pl.ds(0, SIDE)
    uvw = pl.ds(0, 3)
    loads = [
        (index_v, index_s),
        (rx, vx),
        (ry, vy),
        (rd, vd),
        (rlow, vlow),
        (rhigh, vhigh),
        (ux_low, fluid.at[uvw, pl.ds(0, 1), inner, :]),
        (ux_high, fluid.at[uvw, pl.ds(SIDE + 1, 2), inner, :]),
        (dx_low, fluid.at[3, pl.ds(0, 1), inner, :]),
        (dx_high, fluid.at[3, pl.ds(SIDE + 1, 2), inner, :]),
        (grid, force),
        (u_old, fluid.at[uvw, pl.ds(1, SIDE), inner, :]),
        (density, fluid.at[3, pl.ds(1, SIDE), inner, :]),
    ]
    copies = [pltpu.make_async_copy(source, target, sems.at[n]) for n, (source, target) in enumerate(loads)]
    for copy in copies:
        copy.start()
    velocity[...] = jnp.zeros_like(velocity)
    build = functools.partial(gather_build, offsets=offsets, base_z=base_z)
    build(jnp.int32(0), across=across_a, along=along_a, depth=depth_a)
    for copy in copies:
        copy.wait()

    for n in range(4):
        right, down = n % 2, n // 2
        for half in range(2):
            where = pl.ds(288 * right, 32)
            vy[down, half, where, :] += vd[n, half]
    for right in range(2):
        for n in range(3):
            force[(SIDE * right) + n] += vx[right, n]

    row = iota((8, LANES), 0)
    last_row = row == 7
    two_rows = row < 2
    inside = jnp.logical_or(last_row, two_rows)

    @pl.loop(0, PLANES)
    def _(x):
        fresh = [[[None, None] for _ in range(3)] for _ in range(5)]
        for half in range(2):
            lanes = slice(half * LANES, (half + 1) * LANES)

            def edge(c):
                high = vhigh[half, pl.ds(x * 4 + c + 5, 8), :]
                low = vlow[half, pl.ds((x * 4 + c) * 2, 8), :]
                return jnp.where(inside, jnp.where(last_row, high, low), 1.0 if c == 3 else 0.0)

            rate = [0.5 / fluid[3, x, 8 * yb : 8 * yb + 8, lanes] for yb in range(4)] + [0.5 / edge(3)]
            for c in range(3):
                push = [force[x, c, 8 * yb : 8 * yb + 8, lanes] for yb in range(5)]
                start = (x * 3 + c) * 3
                below = pltpu.roll(vy[0, half, pl.ds(start, 8), :], 7, 0)
                above = pltpu.roll(vy[1, half, pl.ds(start, 8), :], 7, 0)
                push[0] = push[0] + jnp.where(two_rows, below, 0.0)
                push[3] = push[3] + jnp.where(last_row, above, 0.0)
                push[4] = jnp.where(inside, push[4] + jnp.where(last_row, below, above), 0.0)
                for yb in range(4):
                    value = fluid[c, x, 8 * yb : 8 * yb + 8, lanes] + push[yb] * rate[yb]
                    fluid[c, x, 8 * yb : 8 * yb + 8, lanes] = value
                    fresh[yb][c][half] = value
                fresh[4][c][half] = edge(c) + push[4] * rate[4]
        packed = []
        for yb in range(5):
            moved = [[pltpu.roll(v, CS * c, 1) if c else v for v in fresh[yb][c]] for c in range(3)]
            tiles = []
            for t in range(NT):
                value = None
                for c in range(3):
                    for half, low, high in segments(t):
                        piece = moved[c][half]
                        value = piece if value is None else jnp.where(lane_mask(c, low, high), piece, value)
                tiles.append(value)
            packed.append(tiles)
        for t in range(NT):
            start = FRONT + (x * NT + t) * BLOCK
            table[pl.ds(start, 8), :] = pltpu.roll(packed[4][t], 1, 0)
            for yb in range(5):
                table[pl.ds(start + 8 * yb + 1, 8), :] = packed[yb][t]

        @pl.when(jnp.logical_and(x > 0, x <= SIDE))
        def _():
            pltpu.make_async_copy(
                fluid.at[uvw, pl.ds(x, 1), inner, :], u_new.at[:, pl.ds(x - 1, 1)], plane_sems.at[x - 1]
            ).start()

    live_tiles = count[0]
    finish = functools.partial(gather_markers, count=live_tiles, index_s=index_s, table=table, velocity=velocity)

    @pl.loop(0, lax.shift_right_logical(live_tiles + 1, 1))
    def _(turn):
        zero = jnp.minimum(turn, 0)
        build(2 * turn + 1, across=across_b, along=along_b, depth=depth_b)
        finish(2 * turn, zero, across=across_a, along=along_a, depth=depth_a, stage=stage_a)
        build(2 * turn + 2, across=across_a, along=along_a, depth=depth_a)
        finish(2 * turn + 1, zero, across=across_b, along=along_b, depth=depth_b, stage=stage_b)

    @pl.loop(0, SIDE)
    def _(x):
        pltpu.make_async_copy(
            fluid.at[uvw, pl.ds(x + 1, 1), inner, :], u_new.at[:, pl.ds(x, 1)], plane_sems.at[x]
        ).wait()


def gather(count, offsets, base_x, base_y, base_z, u_old, density, grid, *received):
    wide = VMEM((LANES, LANES), F32)
    return pl.pallas_call(
        gather_kernel,
        name="gather",
        in_specs=[pl.BlockSpec(memory_space=SMEM)]
        + [pl.BlockSpec(memory_space=VMEM)] * 4
        + [pl.BlockSpec(memory_space=HBM)] * (3 + len(EXCHANGED)),
        out_specs=[pl.BlockSpec(memory_space=HBM), pl.BlockSpec(memory_space=VMEM)],
        out_shape=[
            jax.ShapeDtypeStruct((3, SIDE, SIDE, NZ), F32),
            jax.ShapeDtypeStruct((3, SLOTS, LANES), F32),
        ],
        scratch_shapes=[
            VMEM((SLOTS, LANES), I32),
            SMEM((SLOTS, LANES), I32),
            VMEM((ROWS, LANES), F32),
            VMEM((4, PLANES, SIDE, NZ), F32),
            VMEM((PLANES, 3, 40, NZ), F32),
        ]
        + [VMEM(shape, F32) for shape in EXCHANGED[:5]]
        + [VMEM((4, LANES, LANES), F32)] * 4
        + [VMEM((3, LANES, LANES), F32)] * 2
        + [VMEM((4 * LANES, LANES), F32)] * 2
        + [pltpu.SemaphoreType.DMA((13,)), pltpu.SemaphoreType.DMA((SIDE,))],
        compiler_params=pltpu.CompilerParams(vmem_limit_bytes=63 * 2**20),
    )(count, offsets, base_x, base_y, base_z, u_old, density, grid, *received)


def on_device(u_old, density, offsets, forces, base_x, base_y, base_z, tile_count):
    grid, strip, low, high = spread(tile_count, offsets, forces, base_x, base_y, base_z, u_old, density)
    received = exchange(grid, strip, low, high, u_old, density)
    return tuple(gather(tile_count, offsets, base_x, base_y, base_z, u_old, density, grid, *received))


def solution(mesh):
    tiles = P(("gx", "gy"), None)
    in_specs = (
        P(None, "gx", "gy", None),
        P("gx", "gy", None),
        P(None, ("gx", "gy"), None),
        P(None, ("gx", "gy"), None),
        tiles,
        tiles,
        tiles,
        P(("gx", "gy")),
    )
    out_specs = (P(None, "gx", "gy", None), P(None, ("gx", "gy"), None))
    return jax.shard_map(on_device, mesh=mesh, in_specs=in_specs, out_specs=out_specs, check_vma=False)
```

```python
import functools

import jax
import jax.numpy as jnp
from jax import lax
from jax.experimental import pallas as pl
from jax.experimental.pallas import tpu as pltpu
from jax.sharding import PartitionSpec as P

F32 = jnp.float32
I32 = jnp.int32
HBM = pltpu.HBM
VMEM = pltpu.VMEM
SMEM = pltpu.SMEM

SLOTS = 16
LANES = 128
SIDE = 32
NZ = 256
NT = 7
ZS, ZW = 37, 40
CS = 42
PLANES = 35
GROUPS = 7
BLOCK = 40
STEP = NT * BLOCK
FRONT = 8
ROWS = 9856
COPIES = 2
PART = 32


def iota(shape, dim):
    return lax.broadcasted_iota(I32, shape, dim)


def four_weights(frac, root):
    low, high = 3.0 - 2.0 * frac, 1.0 + 2.0 * frac
    return [(low - root) * 0.125, (low + root) * 0.125, (high + root) * 0.125, (high - root) * 0.125]


def root_of(frac):
    return jnp.sqrt(1.0 + 4.0 * frac - 4.0 * frac * frac)


def row_index(bx, by, bz):
    z_tile = lax.shift_right_logical(bz * 1772, 16)
    return (bx * NT + z_tile) * BLOCK + by + FRONT


def columns_of(rows):
    rows = rows + [rows[-1]] * (-len(rows) % 8)
    return jnp.concatenate(rows, axis=0).T


def depth_weights(place, frac, root):
    away = iota((8, LANES), 1).astype(F32) - place
    away = jnp.where(away < 0.0, away + 128.0, away)
    first, second = away < CS - 0.5, away < 2 * CS - 0.5
    k = away - jnp.where(first, 0.0, jnp.where(second, float(CS), float(2 * CS)))
    value = jnp.where(k < 1.5, 3.0 - 2.0 * frac, 1.0 + 2.0 * frac)
    value = (value + jnp.where(jnp.abs(k - 1.5) < 1.0, root, -root)) * 0.125
    value = jnp.where(k < 3.5, value, 0.0)
    later = jnp.where(first, 0.0, value)
    return [jnp.where(first, value, 0.0), jnp.where(second, later, 0.0), jnp.where(second, 0.0, later)]


def z_place(bz):
    return lax.bitwise_and(bz + 127, 127).astype(F32)


def segments(t):
    found = []
    for half in range(2):
        for turn in (-1, 0, 1):
            low = max(ZS * t - 1 + NZ * turn - LANES * half, 0)
            high = min(ZS * t - 1 + ZW + NZ * turn - LANES * half, LANES)
            if low < high:
                found.append((half, low, high))
    return found


def lane_mask(c, low, high):
    lane = lax.bitwise_and(iota((8, LANES), 1) + (LANES - CS * c), 127)
    if low == 0:
        return lane < high
    if high == LANES:
        return lane >= low
    return jnp.logical_and(lane >= low, lane < high)


def spread_columns(tile, count, offsets, forces, base_z):
    live = jnp.where(tile < count, 1.0, 0.0)
    sx, sy, sz = (offsets[i, pl.ds(tile, 1), :] for i in range(3))
    push = [forces[c, pl.ds(tile, 1), :] * live for c in range(3)]
    return columns_of(
        [z_place(base_z[pl.ds(tile, 1), :]), sz, root_of(sz)] + push + [sy, root_of(sy), sx, root_of(sx)]
    )


def spread_wide(tables, tile, g):
    rows = tables[jnp.minimum(tile, SLOTS - 1), pl.ds(pl.multiple_of(8 * g, 8), 8), :]
    return [jnp.broadcast_to(rows[:, n : n + 1], (8, LANES)) for n in range(10)]


def spread_store(wide, g, line, across):
    depth = sum(w * part for w, part in zip(wide[3:6], depth_weights(*wide[:3])))
    for b, weight in enumerate(four_weights(wide[6], wide[7])):
        line[pl.ds(g * 32 + b, 8, stride=4), :] = weight * depth
    for a, weight in enumerate(four_weights(wide[8], wide[9])):
        across[a, pl.ds(pl.multiple_of(8 * g, 8), 8), :] = weight


def spread_group(tile, part, zero, first, index_s, line, across, grids):
    made = []
    for n in range(COPIES):
        m = first + n
        start = index_s[part, tile, m]
        rows = line[pl.ds(zero + m * 4, 4), :]
        for a in range(4):
            where = pl.ds(start + a * STEP, 4)
            weight = jnp.broadcast_to(across[a, m : m + 1, :], (4, LANES))
            made.append((grids[n], where, grids[n][where, :] + weight * rows))
    for grid, where, value in made:
        grid[where, :] = value


def spread_kernel(
    count, offsets, forces, base_x, base_y, base_z, u_old, density,
    grid_out, strip_out, low_out, high_out,
    *scratch,
):
    grids = scratch[:COPIES]
    (index_v, index_s, tables, line_a, line_b, across_a, across_b, planes, strips, edge_low, edge_high, low_v, high_v,
     sems, plane_sems) = scratch[COPIES:]
    index = row_index(base_x[...], base_y[...], base_z[...])
    for part in range(LANES // PART):
        index_v[part] = pltpu.roll(index, LANES - PART * part, 1) if part else index
    to_smem = pltpu.make_async_copy(index_v, index_s, sems.at[0])
    to_smem.start()
    edges = []
    for n, (first, place) in enumerate(((0, edge_low), (SIDE - 8, edge_high))):
        edges.append(pltpu.make_async_copy(u_old.at[:, :, pl.ds(first, 8), :], place.at[pl.ds(0, 3)], sems.at[1 + 2 * n]))
        edges.append(pltpu.make_async_copy(density.at[:, pl.ds(first, 8), :], place.at[3], sems.at[2 + 2 * n]))
    for copy in edges:
        copy.start()

    live_tiles = count[0]
    columns = functools.partial(spread_columns, count=live_tiles, offsets=offsets, forces=forces, base_z=base_z)
    for tile in range(SLOTS):
        tables[tile] = columns(tile)
    for g in range(LANES // 8):
        spread_store(spread_wide(tables, 0, g), g, line_a, across_a)
    nothing = jnp.zeros((8, LANES), F32)

    @pl.loop(0, ROWS // 64)
    def _(i):
        for grid in grids:
            for j in range(8):
                grid[pl.ds(i * 64 + j * 8, 8), :] = nothing

    to_smem.wait()

    @pl.loop(0, lax.shift_right_logical(live_tiles + 1, 1))
    def _(turn):
        for n, (now, later) in enumerate((((line_a, across_a), (line_b, across_b)), ((line_b, across_b), (line_a, across_a)))):
            tile = 2 * turn + n

            @pl.loop(0, LANES // PART)
            def _(part):
                chunks = [part * (PART // 8) + j for j in range(PART // 8)]
                wide = [spread_wide(tables, tile + 1, g) for g in chunks]
                line = now[0].at[pl.ds(pl.multiple_of(part * 4 * PART, 8), 4 * PART), :]
                across = now[1].at[:, pl.ds(pl.multiple_of(part * PART, 8), PART), :]
                for first in range(0, PART, COPIES):
                    spread_group(tile, part, jnp.minimum(part, 0), first, index_s, line, across, grids)
                for g, values in zip(chunks, wide):
                    spread_store(values, g, *later)

    for copy in edges:
        copy.wait()
    row = iota((8, LANES), 0)
    three_rows = row < 3

    @pl.loop(0, SIDE)
    def _(x):
        for half in range(2):
            lanes = slice(half * LANES, (half + 1) * LANES)
            for c in range(4):
                low_v[half, pl.ds((x * 4 + c) * 2, 8), :] = edge_low[c, x, :, lanes]
                high_v[half, pl.ds(x * 4 + c, 8), :] = pltpu.roll(edge_high[c, x, :, lanes], 1, 0)

    def plane_copy(k):
        return pltpu.make_async_copy(planes.at[pl.ds(5 * k, 5)], grid_out.at[pl.ds(5 * k, 5)], plane_sems.at[k])

    @pl.loop(0, PLANES // 5)
    def _(k):
        for i in range(5):
            x = 5 * k + i
            for yb in range(5):
                tiles = []
                for t in range(NT):
                    start = pl.multiple_of(FRONT + (x * NT + t) * BLOCK, 8) + 8 * yb
                    tiles.append(sum(grid[pl.ds(pl.multiple_of(start, 8), 8), :] for grid in grids))
                for c in range(3):
                    for half in range(2):
                        total = None
                        for group in ((0, 2, 4), (1, 3, 5), (6,)):
                            part = None
                            for t in group:
                                for at, low, high in segments(t):
                                    if at == half:
                                        part = jnp.where(lane_mask(c, low, high), tiles[t], 0.0 if part is None else part)
                            if part is not None:
                                total = part if total is None else total + part
                        if c:
                            total = pltpu.roll(total, LANES - CS * c, 1)
                        planes[x, c, half, 8 * yb : 8 * yb + 8, :] = total
                        if yb in (0, 4):
                            strips[yb // 4, half, pl.ds((x * 3 + c) * 3, 8), :] = jnp.where(three_rows, total, 0.0)

        plane_copy(k).start()

    tail = [
        pltpu.make_async_copy(strips, strip_out, sems.at[0]),
        pltpu.make_async_copy(low_v, low_out, sems.at[1]),
        pltpu.make_async_copy(high_v, high_out, sems.at[2]),
    ]
    for copy in tail:
        copy.start()
    for copy in tail:
        copy.wait()
    for k in range(PLANES // 5):
        plane_copy(k).wait()


LOW_ROWS = 264
HIGH_ROWS = 136
YROWS = 320


def spread(count, offsets, forces, base_x, base_y, base_z, u_old, density):
    return pl.pallas_call(
        spread_kernel,
        name="spread",
        in_specs=[pl.BlockSpec(memory_space=SMEM)] + [pl.BlockSpec(memory_space=VMEM)] * 5 + [pl.BlockSpec(memory_space=HBM)] * 2,
        out_specs=[pl.BlockSpec(memory_space=HBM)] * 4,
        out_shape=[
            jax.ShapeDtypeStruct((PLANES, 3, 2, 40, LANES), F32),
            jax.ShapeDtypeStruct((2, 2, YROWS, LANES), F32),
            jax.ShapeDtypeStruct((2, LOW_ROWS, LANES), F32),
            jax.ShapeDtypeStruct((2, HIGH_ROWS, LANES), F32),
        ],
        scratch_shapes=[VMEM((ROWS, LANES), F32)] * COPIES
        + [VMEM((LANES // PART, SLOTS, LANES), I32), SMEM((LANES // PART, SLOTS, LANES), I32)]
        + [VMEM((SLOTS, LANES, 16), F32)]
        + [VMEM((4 * LANES, LANES), F32)] * 2
        + [VMEM((4, LANES, LANES), F32)] * 2
        + [
            VMEM((PLANES, 3, 2, 40, LANES), F32),
            VMEM((2, 2, YROWS, LANES), F32),
            VMEM((4, SIDE, 8, NZ), F32),
            VMEM((4, SIDE, 8, NZ), F32),
            VMEM((2, LOW_ROWS, LANES), F32),
            VMEM((2, HIGH_ROWS, LANES), F32),
            pltpu.SemaphoreType.DMA((5,)),
            pltpu.SemaphoreType.DMA((PLANES // 5,)),
        ],
        compiler_params=pltpu.CompilerParams(vmem_limit_bytes=63 * 2**20),
    )(count, offsets, forces, base_x, base_y, base_z, u_old, density)


def exchange_kernel(
    grid, strip, low, high, u_old, density,
    rx, ry, rd, rlow, rhigh, ux_low, ux_high, dx_low, dx_high,
    send_sems, recv_sems,
):
    nx, ny = lax.axis_size("gx"), lax.axis_size("gy")
    gx, gy = lax.axis_index("gx"), lax.axis_index("gy")
    left, right = lax.rem(gx + nx - 1, nx), lax.rem(gx + 1, nx)
    down, up = lax.rem(gy + ny - 1, ny), lax.rem(gy + 1, ny)
    around = [(i, j) for i in (left, gx, right) for j in (down, gy, up)]
    del around[4]
    barrier = pltpu.get_barrier_semaphore()
    for place in around:
        pl.semaphore_signal(barrier, inc=1, device_id=place, device_id_type=pl.DeviceIdType.MESH)
    pl.semaphore_wait(barrier, len(around))
    last = pl.ds(SIDE - 1, 1)
    first = pl.ds(0, 2)
    rows = lambda start, size: pl.ds(start, size)
    moves = [
        (strip.at[1, :, rows(0, 320), :], ry.at[0], (gx, up)),
        (strip.at[0, :, rows(0, 320), :], ry.at[1], (gx, down)),
        (low.at[:, rows(0, 256), :], rlow.at[:, rows(8, 256), :], (gx, down)),
        (high.at[:, rows(0, 128), :], rhigh.at[:, rows(16, 128), :], (gx, up)),
        (grid.at[rows(SIDE, 3)], rx.at[0], (right, gy)),
        (grid.at[rows(0, 3)], rx.at[1], (left, gy)),
        (u_old.at[:, last], ux_low, (right, gy)),
        (u_old.at[:, first], ux_high, (left, gy)),
        (density.at[last], dx_low, (right, gy)),
        (density.at[first], dx_high, (left, gy)),
        (strip.at[1, :, rows(288, 32), :], rd.at[0], (right, up)),
        (high.at[:, rows(120, 8), :], rhigh.at[:, rows(8, 8), :], (right, up)),
        (strip.at[1, :, rows(0, 32), :], rd.at[1], (left, up)),
        (high.at[:, rows(0, 8), :], rhigh.at[:, rows(144, 8), :], (left, up)),
        (strip.at[0, :, rows(288, 32), :], rd.at[2], (right, down)),
        (low.at[:, rows(248, 8), :], rlow.at[:, rows(0, 8), :], (right, down)),
        (strip.at[0, :, rows(0, 32), :], rd.at[3], (left, down)),
        (low.at[:, rows(0, 16), :], rlow.at[:, rows(264, 16), :], (left, down)),
    ]
    copies = [
        pltpu.make_async_remote_copy(
            src_ref=source,
            dst_ref=target,
            send_sem=send_sems.at[n],
            recv_sem=recv_sems.at[n],
            device_id=place,
            device_id_type=pl.DeviceIdType.MESH,
        )
        for n, (source, target, place) in enumerate(moves)
    ]
    for copy in copies:
        copy.start()
    for copy in copies:
        copy.wait()


MOVES = 18
RLOW_ROWS, RHIGH_ROWS = 296, 160
EXCHANGED = (
    (2, 3, 3, 2, 40, LANES),
    (2, 2, 320, LANES),
    (4, 2, 32, LANES),
    (2, RLOW_ROWS, LANES),
    (2, RHIGH_ROWS, LANES),
    (3, 1, SIDE, NZ),
    (3, 2, SIDE, NZ),
    (1, SIDE, NZ),
    (2, SIDE, NZ),
)


def exchange(grid, strip, low, high, u_old, density):
    return pl.pallas_call(
        exchange_kernel,
        name="exchange",
        in_specs=[pl.BlockSpec(memory_space=HBM)] * 6,
        out_specs=[pl.BlockSpec(memory_space=HBM)] * len(EXCHANGED),
        out_shape=[jax.ShapeDtypeStruct(shape, F32) for shape in EXCHANGED],
        scratch_shapes=[pltpu.SemaphoreType.DMA((MOVES,)), pltpu.SemaphoreType.DMA((MOVES,))],
        compiler_params=pltpu.CompilerParams(collective_id=0, has_side_effects=True),
    )(grid, strip, low, high, u_old, density)


def gather_build(tile, offsets, base_z, across, along, depth):
    sx, sy, sz = (offsets[i, pl.ds(tile, 1), :] for i in range(3))
    table = columns_of([z_place(base_z[pl.ds(tile, 1), :]), sz, root_of(sz), sy, root_of(sy), sx, root_of(sx)])
    for g in range(LANES // 8):
        rows = slice(8 * g, 8 * g + 8)
        wide = [jnp.broadcast_to(table[rows, n : n + 1], (8, LANES)) for n in range(7)]
        for c, value in enumerate(depth_weights(wide[0], wide[1], wide[2])):
            depth[c, rows, :] = value
        for b, weight in enumerate(four_weights(wide[3], wide[4])):
            along[b, rows, :] = weight
        for a, weight in enumerate(four_weights(wide[5], wide[6])):
            across[a, rows, :] = weight


def gather_markers(tile, zero, count, index_s, table, across, along, depth, stage, velocity):
    for m in range(LANES):
        start = index_s[tile, m]
        total = None
        for a in range(4):
            term = jnp.broadcast_to(across[a, m : m + 1, :], (4, LANES)) * table[pl.ds(start + a * STEP, 4), :]
            total = term if total is None else total + term
        stage[pl.ds(zero + m * 4, 4), :] = total
    picked = [[] for _ in range(3)]
    for g in range(LANES // 8):
        rows = slice(8 * g, 8 * g + 8)
        total = None
        for b in range(4):
            term = along[b, rows, :] * stage[pl.ds(zero + g * 32 + b, 8, stride=4), :]
            total = term if total is None else total + term
        for c in range(3):
            picked[c].append(total * depth[c, rows, :])
    values = jnp.concatenate(picked[0] + picked[1] + picked[2], axis=0)
    rough = values.astype(jnp.bfloat16)
    rest = (values - rough.astype(F32)).astype(jnp.bfloat16)
    both = jnp.concatenate([rough, rest], axis=1)
    out = lax.dot_general(
        jnp.ones((8, 2 * LANES), jnp.bfloat16), both, (((1,), (1,)), ((), ())), preferred_element_type=F32
    )
    for c in range(3):
        velocity[c, pl.ds(tile, 1), :] = jnp.where(tile < count, out[0:1, c * LANES : (c + 1) * LANES], 0.0)


def gather_kernel(
    count, offsets, base_x, base_y, base_z, u_old, density, grid,
    rx, ry, rd, rlow, rhigh, ux_low, ux_high, dx_low, dx_high,
    u_new, velocity,
    index_v, index_s, table, fluid, force, vx, vy, vd, vlow, vhigh,
    across, along, depth, stage_a, stage_b, sems, force_sems, old_sems, new_sems,
):
    inner = pl.ds(0, SIDE)
    uvw = pl.ds(0, 3)
    loads = [
        (rx, vx),
        (ry, vy),
        (rd, vd),
        (rlow, vlow),
        (rhigh, vhigh),
        (ux_low, fluid.at[uvw, pl.ds(0, 1), inner, :]),
        (ux_high, fluid.at[uvw, pl.ds(SIDE + 1, 2), inner, :]),
        (dx_low, fluid.at[3, pl.ds(0, 1), inner, :]),
        (dx_high, fluid.at[3, pl.ds(SIDE + 1, 2), inner, :]),
    ]
    copies = [pltpu.make_async_copy(source, target, sems.at[1 + n]) for n, (source, target) in enumerate(loads)]
    for copy in copies:
        copy.start()

    def force_copy(k):
        return pltpu.make_async_copy(grid.at[pl.ds(5 * k, 5)], force.at[pl.ds(5 * k, 5)], force_sems.at[k])

    def old_copies(k, first, size):
        here, there = pl.ds(first, size), pl.ds(first + 1, size)
        return (
            pltpu.make_async_copy(u_old.at[:, here], fluid.at[uvw, there, inner, :], old_sems.at[0, k]),
            pltpu.make_async_copy(density.at[here], fluid.at[3, there, inner, :], old_sems.at[1, k]),
        )

    def new_copy(k, first, size):
        return pltpu.make_async_copy(
            fluid.at[uvw, pl.ds(first + 1, size), inner, :], u_new.at[:, pl.ds(first, size)], new_sems.at[k]
        )

    def span(k):
        first, last = max(5 * k - 1, 0), min(5 * k + 4, SIDE)
        return first, last - first

    def each_span(k, act):
        pl.when(k == 0)(lambda: act(k, *span(0)))
        pl.when(k == GROUPS - 1)(lambda: act(k, *span(GROUPS - 1)))
        pl.when(jnp.logical_and(k > 0, k < GROUPS - 1))(lambda: act(k, 5 * k - 1, 5))

    def wait_old(*where):
        for copy in old_copies(*where):
            copy.wait()

    def start_new(*where):
        new_copy(*where).start()

    stages = (stage_a, stage_b)
    for k in range(GROUPS):
        force_copy(k).start()
        for copy in old_copies(k, *span(k)):
            copy.start()
    index_v[...] = row_index(base_x[...], base_y[...], base_z[...])
    to_smem = pltpu.make_async_copy(index_v, index_s, sems.at[0])
    to_smem.start()
    velocity[...] = jnp.zeros_like(velocity)
    live_tiles = count[0]

    pairs = lax.shift_right_logical(live_tiles + 1, 1)

    @pl.loop(0, pairs)
    def _(turn):
        for tile in (2 * turn, 2 * turn + 1):
            gather_build(tile, offsets, base_z, across.at[tile], along.at[tile], depth.at[tile])

    to_smem.wait()
    for copy in copies:
        copy.wait()
    for n in range(4):
        right, down = n % 2, n // 2
        for half in range(2):
            where = pl.ds(288 * right, 32)
            vy[down, half, where, :] += vd[n, half]

    row = iota((8, LANES), 0)
    first_row, last_row = row == 0, row == 7
    two_rows = row < 2
    inside = jnp.logical_or(last_row, two_rows)

    def plane(x, zero):
        fresh = [[[None, None] for _ in range(3)] for _ in range(5)]
        for half in range(2):
            lanes = slice(half * LANES, (half + 1) * LANES)

            def edge(c):
                high = vhigh[half, pl.ds(x * 4 + c + 5, 8), :]
                low = vlow[half, pl.ds((x * 4 + c) * 2, 8), :]
                return jnp.where(inside, jnp.where(last_row, high, low), 1.0 if c == 3 else 0.0)

            rate = [0.5 / fluid[3, x, 8 * yb : 8 * yb + 8, lanes] for yb in range(4)] + [0.5 / edge(3)]
            for c in range(3):
                push = [force[x, c, half, pl.ds(zero + 8 * yb + 1, 8), :] for yb in range(4)]
                where = pl.ds((x * 3 + c) * 3, 8)
                below = pltpu.roll(vy[0, half, where, :], 7, 0)
                above = pltpu.roll(vy[1, half, where, :], 7, 0)
                push[0] = push[0] + jnp.where(two_rows, below, 0.0)
                push[3] = push[3] + jnp.where(last_row, above, 0.0)
                for yb in range(4):
                    value = fluid[c, x, 8 * yb : 8 * yb + 8, lanes] + push[yb] * rate[yb]
                    fluid[c, x, 8 * yb : 8 * yb + 8, lanes] = value
                    fresh[yb][c][half] = value
                outer = pltpu.roll(jnp.where(first_row, force[x, c, half, 0:8, :], force[x, c, half, 32:40, :]), 7, 0)
                outer = jnp.where(inside, outer + jnp.where(last_row, below, above), 0.0)
                fresh[4][c][half] = edge(c) + outer * rate[4]
        packed = []
        for yb in range(5):
            moved = [[pltpu.roll(v, CS * c, 1) if c else v for v in fresh[yb][c]] for c in range(3)]
            tiles = []
            for t in range(NT):
                value = None
                for c in range(3):
                    for half, low, high in segments(t):
                        piece = moved[c][half]
                        value = piece if value is None else jnp.where(lane_mask(c, low, high), piece, value)
                tiles.append(value)
            packed.append(tiles)
        for t in range(NT):
            start = FRONT + (x * NT + t) * BLOCK
            table[pl.ds(start, 8), :] = pltpu.roll(packed[4][t], 1, 0)
            for yb in range(5):
                table[pl.ds(start + 8 * yb + 1, 8), :] = packed[yb][t]

    @pl.loop(0, GROUPS)
    def _(k):
        force_copy(k).wait()
        each_span(k, wait_old)

        @pl.when(k == 0)
        def _():
            for n in range(3):
                force[n] += vx[0, n]

        @pl.when(k == GROUPS - 1)
        def _():
            for n in range(3):
                force[SIDE + n] += vx[1, n]

        zero = jnp.minimum(k, 0)
        for i in range(5):
            plane(5 * k + i, zero)
        each_span(k, start_new)

    @pl.loop(0, pairs)
    def _(turn):
        zero = jnp.minimum(turn, 0)
        for n in range(2):
            tile = 2 * turn + n
            gather_markers(
                tile, zero, live_tiles, index_s, table, across.at[tile], along.at[tile], depth.at[tile], stages[n], velocity
            )

    for k in range(GROUPS):
        new_copy(k, *span(k)).wait()


def gather(count, offsets, base_x, base_y, base_z, u_old, density, grid, *received):
    return pl.pallas_call(
        gather_kernel,
        name="gather",
        in_specs=[pl.BlockSpec(memory_space=SMEM)]
        + [pl.BlockSpec(memory_space=VMEM)] * 4
        + [pl.BlockSpec(memory_space=HBM)] * (3 + len(EXCHANGED)),
        out_specs=[pl.BlockSpec(memory_space=HBM), pl.BlockSpec(memory_space=VMEM)],
        out_shape=[
            jax.ShapeDtypeStruct((3, SIDE, SIDE, NZ), F32),
            jax.ShapeDtypeStruct((3, SLOTS, LANES), F32),
        ],
        scratch_shapes=[
            VMEM((SLOTS, LANES), I32),
            SMEM((SLOTS, LANES), I32),
            VMEM((ROWS, LANES), F32),
            VMEM((4, PLANES, SIDE, NZ), F32),
            VMEM((PLANES, 3, 2, 40, LANES), F32),
        ]
        + [VMEM(shape, F32) for shape in EXCHANGED[:5]]
        + [
            VMEM((SLOTS, 4, LANES, LANES), F32),
            VMEM((SLOTS, 4, LANES, LANES), F32),
            VMEM((SLOTS, 3, LANES, LANES), F32),
            VMEM((4 * LANES, LANES), F32),
            VMEM((4 * LANES, LANES), F32),
            pltpu.SemaphoreType.DMA((10,)),
            pltpu.SemaphoreType.DMA((7,)),
            pltpu.SemaphoreType.DMA((2, GROUPS)),
            pltpu.SemaphoreType.DMA((GROUPS,)),
        ],
        compiler_params=pltpu.CompilerParams(vmem_limit_bytes=63 * 2**20),
    )(count, offsets, base_x, base_y, base_z, u_old, density, grid, *received)


def on_device(u_old, density, offsets, forces, base_x, base_y, base_z, tile_count):
    grid, strip, low, high = spread(tile_count, offsets, forces, base_x, base_y, base_z, u_old, density)
    received = exchange(grid, strip, low, high, u_old, density)
    return tuple(gather(tile_count, offsets, base_x, base_y, base_z, u_old, density, grid, *received))


def solution(mesh):
    tiles = P(("gx", "gy"), None)
    in_specs = (
        P(None, "gx", "gy", None),
        P("gx", "gy", None),
        P(None, ("gx", "gy"), None),
        P(None, ("gx", "gy"), None),
        tiles,
        tiles,
        tiles,
        P(("gx", "gy")),
    )
    out_specs = (P(None, "gx", "gy", None), P(None, ("gx", "gy"), None))
    return jax.shard_map(on_device, mesh=mesh, in_specs=in_specs, out_specs=out_specs, check_vma=False)
```

```python
import functools

import jax
import jax.numpy as jnp
from jax import lax
from jax.experimental import pallas as pl
from jax.experimental.pallas import tpu as pltpu
from jax.sharding import PartitionSpec as P

F32 = jnp.float32
I32 = jnp.int32
HBM = pltpu.HBM
VMEM = pltpu.VMEM
SMEM = pltpu.SMEM

SLOTS = 16
LANES = 128
SIDE = 32
NZ = 256
NT = 7
ZS, ZW = 37, 40
CS = 42
PLANES = 35
GROUPS = 7
BLOCK = 40
STEP = NT * BLOCK
FRONT = 8
ROWS = 9856
COPIES = 2
PART = 32


def iota(shape, dim):
    return lax.broadcasted_iota(I32, shape, dim)


def four_weights(frac, root):
    low, high = 3.0 - 2.0 * frac, 1.0 + 2.0 * frac
    return [(low - root) * 0.125, (low + root) * 0.125, (high + root) * 0.125, (high - root) * 0.125]


def root_of(frac):
    return jnp.sqrt(1.0 + 4.0 * frac - 4.0 * frac * frac)


def row_index(bx, by, bz):
    z_tile = lax.shift_right_logical(bz * 1772, 16)
    return (bx * NT + z_tile) * BLOCK + by + FRONT


def columns_of(rows):
    rows = rows + [rows[-1]] * (-len(rows) % 8)
    return jnp.concatenate(rows, axis=0).T


def depth_weights(place, frac, root):
    away = iota((8, LANES), 1).astype(F32) - place
    away = jnp.where(away < 0.0, away + 128.0, away)
    first, second = away < CS - 0.5, away < 2 * CS - 0.5
    k = away - jnp.where(first, 0.0, jnp.where(second, float(CS), float(2 * CS)))
    value = jnp.where(k < 1.5, 3.0 - 2.0 * frac, 1.0 + 2.0 * frac)
    value = (value + jnp.where(jnp.abs(k - 1.5) < 1.0, root, -root)) * 0.125
    value = jnp.where(k < 3.5, value, 0.0)
    later = jnp.where(first, 0.0, value)
    return [jnp.where(first, value, 0.0), jnp.where(second, later, 0.0), jnp.where(second, 0.0, later)]


def z_place(bz):
    return lax.bitwise_and(bz + 127, 127).astype(F32)


def segments(t):
    found = []
    for half in range(2):
        for turn in (-1, 0, 1):
            low = max(ZS * t - 1 + NZ * turn - LANES * half, 0)
            high = min(ZS * t - 1 + ZW + NZ * turn - LANES * half, LANES)
            if low < high:
                found.append((half, low, high))
    return found


def lane_mask(c, low, high):
    lane = lax.bitwise_and(iota((8, LANES), 1) + (LANES - CS * c), 127)
    if low == 0:
        return lane < high
    if high == LANES:
        return lane >= low
    return jnp.logical_and(lane >= low, lane < high)


def spread_columns(tile, count, offsets, forces, base_z):
    live = jnp.where(tile < count, 1.0, 0.0)
    sx, sy, sz = (offsets[i, pl.ds(tile, 1), :] for i in range(3))
    push = [forces[c, pl.ds(tile, 1), :] * live for c in range(3)]
    return columns_of(
        [z_place(base_z[pl.ds(tile, 1), :]), sz, root_of(sz)] + push + [sy, root_of(sy), sx, root_of(sx)]
    )


def spread_wide(tables, tile, g):
    rows = tables[jnp.minimum(tile, SLOTS - 1), pl.ds(pl.multiple_of(8 * g, 8), 8), :]
    return [jnp.broadcast_to(rows[:, n : n + 1], (8, LANES)) for n in range(10)]


def spread_store(wide, g, line, across):
    depth = sum(w * part for w, part in zip(wide[3:6], depth_weights(*wide[:3])))
    for b, weight in enumerate(four_weights(wide[6], wide[7])):
        line[pl.ds(g * 32 + b, 8, stride=4), :] = weight * depth
    for a, weight in enumerate(four_weights(wide[8], wide[9])):
        across[a, pl.ds(pl.multiple_of(8 * g, 8), 8), :] = weight


def spread_group(tile, part, zero, first, index_s, line, across, grids):
    made = []
    for n in range(COPIES):
        m = first + n
        start = index_s[part, tile, m]
        rows = line[pl.ds(zero + m * 4, 4), :]
        for a in range(4):
            where = pl.ds(start + a * STEP, 4)
            weight = jnp.broadcast_to(across[a, m : m + 1, :], (4, LANES))
            made.append((grids[n], where, grids[n][where, :] + weight * rows))
    for grid, where, value in made:
        grid[where, :] = value


def spread_kernel(
    count, offsets, forces, base_x, base_y, base_z, u_old, density,
    grid_out, strip_out, low_out, high_out, side_out,
    *scratch,
):
    grids = scratch[:COPIES]
    (index_v, index_s, tables, line_a, line_b, across_a, across_b, planes, strips, edge_low, edge_high, low_v, high_v,
     side_u, side_v, sems, plane_sems) = scratch[COPIES:]
    index = row_index(base_x[...], base_y[...], base_z[...])
    for part in range(LANES // PART):
        index_v[part] = pltpu.roll(index, LANES - PART * part, 1) if part else index
    to_smem = pltpu.make_async_copy(index_v, index_s, sems.at[0])
    to_smem.start()
    inner, uvw = pl.ds(1, SIDE), pl.ds(0, 3)
    edges = []
    for first, place in ((0, edge_low), (SIDE - 8, edge_high)):
        edges.append((u_old.at[:, :, pl.ds(first, 8), :], place.at[uvw, inner]))
        edges.append((density.at[:, pl.ds(first, 8), :], place.at[3, inner]))
    for first, size, at in ((0, 2, 0), (SIDE - 1, 1, 2)):
        edges.append((u_old.at[:, pl.ds(first, size)], side_u.at[uvw, pl.ds(at, size)]))
        edges.append((density.at[pl.ds(first, size)], side_u.at[3, pl.ds(at, size)]))
    edges = [pltpu.make_async_copy(source, target, sems.at[1 + n]) for n, (source, target) in enumerate(edges)]
    for copy in edges:
        copy.start()

    live_tiles = count[0]
    columns = functools.partial(spread_columns, count=live_tiles, offsets=offsets, forces=forces, base_z=base_z)
    for tile in range(SLOTS):
        tables[tile] = columns(tile)
    for g in range(LANES // 8):
        spread_store(spread_wide(tables, 0, g), g, line_a, across_a)
    nothing = jnp.zeros((8, LANES), F32)

    @pl.loop(0, ROWS // 64)
    def _(i):
        for grid in grids:
            for j in range(8):
                grid[pl.ds(i * 64 + j * 8, 8), :] = nothing

    to_smem.wait()

    @pl.loop(0, lax.shift_right_logical(live_tiles + 1, 1))
    def _(turn):
        for n, (now, later) in enumerate((((line_a, across_a), (line_b, across_b)), ((line_b, across_b), (line_a, across_a)))):
            tile = 2 * turn + n

            @pl.loop(0, LANES // PART)
            def _(part):
                chunks = [part * (PART // 8) + j for j in range(PART // 8)]
                wide = [spread_wide(tables, tile + 1, g) for g in chunks]
                line = now[0].at[pl.ds(pl.multiple_of(part * 4 * PART, 8), 4 * PART), :]
                across = now[1].at[:, pl.ds(pl.multiple_of(part * PART, 8), PART), :]
                for first in range(0, PART, COPIES):
                    spread_group(tile, part, jnp.minimum(part, 0), first, index_s, line, across, grids)
                for g, values in zip(chunks, wide):
                    spread_store(values, g, *later)

    for copy in edges:
        copy.wait()
    row = iota((8, LANES), 0)
    three_rows = row < 3
    own_rows = (jnp.logical_or(row == 1, row == 2), row == 0)

    @pl.loop(0, SIDE)
    def _(x):
        for half in range(2):
            lanes = slice(half * LANES, (half + 1) * LANES)
            low_v[half, pl.ds(x * 2, 8), :] = edge_low[3, x + 1, :, lanes]
            high_v[half, pl.ds(x, 8), :] = pltpu.roll(edge_high[3, x + 1, :, lanes], 1, 0)

    def plane_copy(k):
        return pltpu.make_async_copy(planes.at[pl.ds(5 * k, 5)], grid_out.at[pl.ds(5 * k, 5)], plane_sems.at[k])

    @pl.loop(0, PLANES // 5)
    def _(k):
        for i in range(5):
            x = 5 * k + i
            ours = jnp.logical_and(x > 0, x <= SIDE)
            for yb in range(5):
                if yb in (0, 4):
                    edge = edge_high if yb else edge_low
                    halves = (slice(0, LANES), slice(LANES, 2 * LANES))
                    rate = [0.5 / pltpu.roll(edge[3, x, :, lanes], 1, 0) for lanes in halves]
                tiles = []
                for t in range(NT):
                    start = pl.multiple_of(FRONT + (x * NT + t) * BLOCK, 8) + 8 * yb
                    tiles.append(sum(grid[pl.ds(pl.multiple_of(start, 8), 8), :] for grid in grids))
                for c in range(3):
                    for half in range(2):
                        total = None
                        for group in ((0, 2, 4), (1, 3, 5), (6,)):
                            part = None
                            for t in group:
                                for at, low, high in segments(t):
                                    if at == half:
                                        part = jnp.where(lane_mask(c, low, high), tiles[t], 0.0 if part is None else part)
                            if part is not None:
                                total = part if total is None else total + part
                        if c:
                            total = pltpu.roll(total, LANES - CS * c, 1)
                        planes[x, c, half, 8 * yb : 8 * yb + 8, :] = total
                        if yb in (0, 4):
                            known = pltpu.roll(edge[c, x, :, halves[half]], 1, 0) + total * rate[half]
                            value = jnp.where(jnp.logical_and(own_rows[yb // 4], ours), known, total)
                            strips[yb // 4, half, pl.ds((x * 3 + c) * 3, 8), :] = jnp.where(three_rows, value, 0.0)

        plane_copy(k).start()

    last_row, first_row = row == 7, row == 0
    for n, (side, at, plane) in enumerate(((0, 1, 0), (0, 2, 1), (1, 0, 2))):
        x = SIDE * side + at

        @pl.loop(0, 2)
        def _(half):
            lanes = pl.ds(pl.multiple_of(half * LANES, LANES), LANES)

            def shifted_rows(c, yb):
                here = side_u[c, plane, 8 * min(yb, 3) : 8 * min(yb, 3) + 8, lanes]
                before = side_u[c, plane, 8 * max(yb - 1, 0) : 8 * max(yb - 1, 0) + 8, lanes]
                return pltpu.roll(jnp.where(last_row, before, here), 1, 0)

            for yb in range(5):
                rows = slice(8 * yb, 8 * yb + 8)
                rate = 0.5 / shifted_rows(3, yb)
                for c in range(3):
                    force = planes[x, c, half, rows, :]
                    value = shifted_rows(c, yb) + force * rate
                    if yb == 0:
                        value = jnp.where(first_row, force, value)
                    if yb == 4:
                        value = jnp.where(first_row, value, force)
                    side_v[side, at, c, half, rows, :] = value

    for side, at in ((0, 0), (1, 1), (1, 2)):

        @pl.loop(0, 3)
        def _(c):
            side_v[side, at, c] = planes[SIDE * side + at, c]

    tail = [
        pltpu.make_async_copy(strips, strip_out, sems.at[0]),
        pltpu.make_async_copy(low_v, low_out, sems.at[1]),
        pltpu.make_async_copy(high_v, high_out, sems.at[2]),
        pltpu.make_async_copy(side_v, side_out, sems.at[3]),
    ]
    for copy in tail:
        copy.start()
    for copy in tail:
        copy.wait()
    for k in range(PLANES // 5):
        plane_copy(k).wait()


LOW_ROWS = 72
HIGH_ROWS = 40
YROWS = 320


def spread(count, offsets, forces, base_x, base_y, base_z, u_old, density):
    return pl.pallas_call(
        spread_kernel,
        name="spread",
        in_specs=[pl.BlockSpec(memory_space=SMEM)] + [pl.BlockSpec(memory_space=VMEM)] * 5 + [pl.BlockSpec(memory_space=HBM)] * 2,
        out_specs=[pl.BlockSpec(memory_space=HBM)] * 5,
        out_shape=[
            jax.ShapeDtypeStruct((PLANES, 3, 2, 40, LANES), F32),
            jax.ShapeDtypeStruct((2, 2, YROWS, LANES), F32),
            jax.ShapeDtypeStruct((2, LOW_ROWS, LANES), F32),
            jax.ShapeDtypeStruct((2, HIGH_ROWS, LANES), F32),
            jax.ShapeDtypeStruct((2, 3, 3, 2, 40, LANES), F32),
        ],
        scratch_shapes=[VMEM((ROWS, LANES), F32)] * COPIES
        + [VMEM((LANES // PART, SLOTS, LANES), I32), SMEM((LANES // PART, SLOTS, LANES), I32)]
        + [VMEM((SLOTS, LANES, 16), F32)]
        + [VMEM((4 * LANES, LANES), F32)] * 2
        + [VMEM((4, LANES, LANES), F32)] * 2
        + [
            VMEM((PLANES, 3, 2, 40, LANES), F32),
            VMEM((2, 2, YROWS, LANES), F32),
            VMEM((4, PLANES, 8, NZ), F32),
            VMEM((4, PLANES, 8, NZ), F32),
            VMEM((2, LOW_ROWS, LANES), F32),
            VMEM((2, HIGH_ROWS, LANES), F32),
            VMEM((4, 3, SIDE, NZ), F32),
            VMEM((2, 3, 3, 2, 40, LANES), F32),
            pltpu.SemaphoreType.DMA((9,)),
            pltpu.SemaphoreType.DMA((PLANES // 5,)),
        ],
        compiler_params=pltpu.CompilerParams(vmem_limit_bytes=63 * 2**20),
    )(count, offsets, forces, base_x, base_y, base_z, u_old, density)


def exchange_kernel(
    side, strip, low, high, density,
    rx, ry, rd, rlow, rhigh, dx_low, dx_high,
    send_sems, recv_sems,
):
    nx, ny = lax.axis_size("gx"), lax.axis_size("gy")
    gx, gy = lax.axis_index("gx"), lax.axis_index("gy")
    left, right = lax.rem(gx + nx - 1, nx), lax.rem(gx + 1, nx)
    down, up = lax.rem(gy + ny - 1, ny), lax.rem(gy + 1, ny)
    around = [(i, j) for i in (left, gx, right) for j in (down, gy, up)]
    del around[4]
    barrier = pltpu.get_barrier_semaphore()
    for place in around:
        pl.semaphore_signal(barrier, inc=1, device_id=place, device_id_type=pl.DeviceIdType.MESH)
    pl.semaphore_wait(barrier, len(around))
    last = pl.ds(SIDE - 1, 1)
    first = pl.ds(0, 2)
    rows = lambda start, size: pl.ds(start, size)
    moves = [
        (strip.at[1, :, rows(0, 320), :], ry.at[0], (gx, up)),
        (strip.at[0, :, rows(0, 320), :], ry.at[1], (gx, down)),
        (low.at[:, rows(0, 64), :], rlow.at[:, rows(8, 64), :], (gx, down)),
        (high.at[:, rows(0, 32), :], rhigh.at[:, rows(8, 32), :], (gx, up)),
        (side.at[1], rx.at[0], (right, gy)),
        (side.at[0], rx.at[1], (left, gy)),
        (density.at[last], dx_low, (right, gy)),
        (density.at[first], dx_high, (left, gy)),
        (strip.at[1, :, rows(288, 32), :], rd.at[0], (right, up)),
        (high.at[:, rows(24, 8), :], rhigh.at[:, rows(0, 8), :], (right, up)),
        (strip.at[1, :, rows(0, 32), :], rd.at[1], (left, up)),
        (high.at[:, rows(0, 8), :], rhigh.at[:, rows(40, 8), :], (left, up)),
        (strip.at[0, :, rows(288, 32), :], rd.at[2], (right, down)),
        (low.at[:, rows(56, 8), :], rlow.at[:, rows(0, 8), :], (right, down)),
        (strip.at[0, :, rows(0, 32), :], rd.at[3], (left, down)),
        (low.at[:, rows(0, 8), :], rlow.at[:, rows(72, 8), :], (left, down)),
    ]
    copies = [
        pltpu.make_async_remote_copy(
            src_ref=source,
            dst_ref=target,
            send_sem=send_sems.at[n],
            recv_sem=recv_sems.at[n],
            device_id=place,
            device_id_type=pl.DeviceIdType.MESH,
        )
        for n, (source, target, place) in enumerate(moves)
    ]
    for copy in copies:
        copy.start()
    for copy in copies:
        copy.wait()


MOVES = 16
RLOW_ROWS, RHIGH_ROWS = 88, 56
EXCHANGED = (
    (2, 3, 3, 2, 40, LANES),
    (2, 2, 320, LANES),
    (4, 2, 32, LANES),
    (2, RLOW_ROWS, LANES),
    (2, RHIGH_ROWS, LANES),
    (1, SIDE, NZ),
    (2, SIDE, NZ),
)


def exchange(side, strip, low, high, density):
    return pl.pallas_call(
        exchange_kernel,
        name="exchange",
        in_specs=[pl.BlockSpec(memory_space=HBM)] * 5,
        out_specs=[pl.BlockSpec(memory_space=HBM)] * len(EXCHANGED),
        out_shape=[jax.ShapeDtypeStruct(shape, F32) for shape in EXCHANGED],
        scratch_shapes=[pltpu.SemaphoreType.DMA((MOVES,)), pltpu.SemaphoreType.DMA((MOVES,))],
        compiler_params=pltpu.CompilerParams(collective_id=0, has_side_effects=True),
    )(side, strip, low, high, density)


def gather_build(tile, offsets, base_z, across, along, depth):
    sx, sy, sz = (offsets[i, pl.ds(tile, 1), :] for i in range(3))
    table = columns_of([z_place(base_z[pl.ds(tile, 1), :]), sz, root_of(sz), sy, root_of(sy), sx, root_of(sx)])
    for g in range(LANES // 8):
        rows = slice(8 * g, 8 * g + 8)
        wide = [jnp.broadcast_to(table[rows, n : n + 1], (8, LANES)) for n in range(7)]
        for c, value in enumerate(depth_weights(wide[0], wide[1], wide[2])):
            depth[c, rows, :] = value
        for b, weight in enumerate(four_weights(wide[3], wide[4])):
            along[b, rows, :] = weight
        for a, weight in enumerate(four_weights(wide[5], wide[6])):
            across[a, rows, :] = weight


def gather_markers(tile, zero, count, index_s, table, across, along, depth, stage, velocity):
    for m in range(LANES):
        start = index_s[tile, m]
        total = None
        for a in range(4):
            term = jnp.broadcast_to(across[a, m : m + 1, :], (4, LANES)) * table[pl.ds(start + a * STEP, 4), :]
            total = term if total is None else total + term
        stage[pl.ds(zero + m * 4, 4), :] = total
    picked = [[] for _ in range(3)]
    for g in range(LANES // 8):
        rows = slice(8 * g, 8 * g + 8)
        total = None
        for b in range(4):
            term = along[b, rows, :] * stage[pl.ds(zero + g * 32 + b, 8, stride=4), :]
            total = term if total is None else total + term
        for c in range(3):
            picked[c].append(total * depth[c, rows, :])
    values = jnp.concatenate(picked[0] + picked[1] + picked[2], axis=0)
    rough = values.astype(jnp.bfloat16)
    rest = (values - rough.astype(F32)).astype(jnp.bfloat16)
    both = jnp.concatenate([rough, rest], axis=1)
    out = lax.dot_general(
        jnp.ones((8, 2 * LANES), jnp.bfloat16), both, (((1,), (1,)), ((), ())), preferred_element_type=F32
    )
    for c in range(3):
        velocity[c, pl.ds(tile, 1), :] = jnp.where(tile < count, out[0:1, c * LANES : (c + 1) * LANES], 0.0)


def gather_kernel(
    count, offsets, base_x, base_y, base_z, u_old, density, grid,
    rx, ry, rd, rlow, rhigh, dx_low, dx_high,
    u_new, velocity,
    index_v, index_s, table, fluid, force, vx, vy, vd, vlow, vhigh, corner,
    across, along, depth, stage_a, stage_b, sems, force_sems, old_sems, new_sems,
):
    inner = pl.ds(0, SIDE)
    uvw = pl.ds(0, 3)
    loads = [
        (rx, vx),
        (ry, vy),
        (rd, vd),
        (rlow, vlow),
        (rhigh, vhigh),
        (dx_low, fluid.at[3, pl.ds(0, 1), inner, :]),
        (dx_high, fluid.at[3, pl.ds(SIDE + 1, 2), inner, :]),
    ]
    copies = [pltpu.make_async_copy(source, target, sems.at[1 + n]) for n, (source, target) in enumerate(loads)]
    for copy in copies:
        copy.start()

    def force_copy(k):
        return pltpu.make_async_copy(grid.at[pl.ds(5 * k, 5)], force.at[pl.ds(5 * k, 5)], force_sems.at[k])

    def old_copies(k, first, size):
        here, there = pl.ds(first, size), pl.ds(first + 1, size)
        return (
            pltpu.make_async_copy(u_old.at[:, here], fluid.at[uvw, there, inner, :], old_sems.at[0, k]),
            pltpu.make_async_copy(density.at[here], fluid.at[3, there, inner, :], old_sems.at[1, k]),
        )

    def new_copy(k, first, size):
        return pltpu.make_async_copy(
            fluid.at[uvw, pl.ds(first + 1, size), inner, :], u_new.at[:, pl.ds(first, size)], new_sems.at[k]
        )

    def span(k):
        first, last = max(5 * k - 1, 0), min(5 * k + 4, SIDE)
        return first, last - first

    def each_span(k, act):
        pl.when(k == 0)(lambda: act(k, *span(0)))
        pl.when(k == GROUPS - 1)(lambda: act(k, *span(GROUPS - 1)))
        pl.when(jnp.logical_and(k > 0, k < GROUPS - 1))(lambda: act(k, 5 * k - 1, 5))

    def wait_old(*where):
        for copy in old_copies(*where):
            copy.wait()

    def start_new(*where):
        new_copy(*where).start()

    stages = (stage_a, stage_b)
    for k in range(GROUPS):
        force_copy(k).start()
        for copy in old_copies(k, *span(k)):
            copy.start()
    index_v[...] = row_index(base_x[...], base_y[...], base_z[...])
    to_smem = pltpu.make_async_copy(index_v, index_s, sems.at[0])
    to_smem.start()
    velocity[...] = jnp.zeros_like(velocity)
    live_tiles = count[0]

    pairs = lax.shift_right_logical(live_tiles + 1, 1)

    @pl.loop(0, pairs)
    def _(turn):
        for tile in (2 * turn, 2 * turn + 1):
            gather_build(tile, offsets, base_z, across.at[tile], along.at[tile], depth.at[tile])

    to_smem.wait()
    for copy in copies:
        copy.wait()
    corner[...] = jnp.zeros_like(corner)
    for n in range(4):
        right, down = n % 2, n // 2
        for half in range(2):
            corner[down, half, pl.ds(288 * right, 32), :] = vd[n, half]

    row = iota((8, LANES), 0)
    first_row, last_row = row == 0, row == 7
    two_rows = row < 2
    inside = jnp.logical_or(last_row, two_rows)

    def plane(x, zero):
        halo = jnp.logical_or(x == 0, x > SIDE)
        fresh = [[[None, None] for _ in range(3)] for _ in range(5)]
        for half in range(2):
            lanes = slice(half * LANES, (half + 1) * LANES)

            edge = jnp.where(last_row, vhigh[half, pl.ds(x, 8), :], vlow[half, pl.ds(x * 2 + 6, 8), :])
            rate = [0.5 / fluid[3, x, 8 * yb : 8 * yb + 8, lanes] for yb in range(4)] + [0.5 / jnp.where(inside, edge, 1.0)]
            for c in range(3):
                push = [force[x, c, half, pl.ds(zero + 8 * yb + 1, 8), :] for yb in range(4)]
                where = pl.ds((x * 3 + c) * 3, 8)
                below, above = (pltpu.roll(vy[n, half, where, :], 7, 0) for n in range(2))
                far_below, far_above = (pltpu.roll(corner[n, half, where, :], 7, 0) for n in range(2))
                push[0] = push[0] + jnp.where(two_rows, below + far_below, 0.0)
                push[3] = push[3] + jnp.where(last_row, above + far_above, 0.0)
                for yb in range(4):
                    value = fluid[c, x, 8 * yb : 8 * yb + 8, lanes] + push[yb] * rate[yb]
                    fluid[c, x, 8 * yb : 8 * yb + 8, lanes] = value
                    fresh[yb][c][half] = value
                outer = pltpu.roll(jnp.where(first_row, force[x, c, half, 0:8, :], force[x, c, half, 32:40, :]), 7, 0)
                near, far = jnp.where(last_row, below, above), jnp.where(last_row, far_below, far_above)
                known, other = jnp.where(halo, far, near), jnp.where(halo, near, far)
                fresh[4][c][half] = jnp.where(inside, known + (outer + other) * rate[4], 0.0)
        packed = []
        for yb in range(5):
            moved = [[pltpu.roll(v, CS * c, 1) if c else v for v in fresh[yb][c]] for c in range(3)]
            tiles = []
            for t in range(NT):
                value = None
                for c in range(3):
                    for half, low, high in segments(t):
                        piece = moved[c][half]
                        value = piece if value is None else jnp.where(lane_mask(c, low, high), piece, value)
                tiles.append(value)
            packed.append(tiles)
        for t in range(NT):
            start = FRONT + (x * NT + t) * BLOCK
            table[pl.ds(start, 8), :] = pltpu.roll(packed[4][t], 1, 0)
            for yb in range(5):
                table[pl.ds(start + 8 * yb + 1, 8), :] = packed[yb][t]

    @pl.loop(0, GROUPS)
    def _(k):
        force_copy(k).wait()
        each_span(k, wait_old)

        def take_side(side, n):
            x = SIDE * side + n
            if (side, n) in ((0, 1), (0, 2), (1, 0)):
                force[x] += vx[side, n]
                return
            zero = jnp.minimum(k, 0)

            @pl.loop(0, 3)
            def _(c):
                for half in range(2):
                    lanes = slice(half * LANES, (half + 1) * LANES)
                    for yb in range(4):
                        fluid[c, x, 8 * yb : 8 * yb + 8, lanes] = vx[side, n, c, half, pl.ds(zero + 8 * yb + 1, 8), :]
                    force[x, c, half, 0:8, :] += jnp.where(first_row, vx[side, n, c, half, 0:8, :], 0.0)
                    force[x, c, half, 32:40, :] += jnp.where(first_row, 0.0, vx[side, n, c, half, 32:40, :])

        @pl.when(k == 0)
        def _():
            for n in range(3):
                take_side(0, n)

        @pl.when(k == GROUPS - 1)
        def _():
            for n in range(3):
                take_side(1, n)

        zero = jnp.minimum(k, 0)
        for i in range(5):
            plane(5 * k + i, zero)
        each_span(k, start_new)

    @pl.loop(0, pairs)
    def _(turn):
        zero = jnp.minimum(turn, 0)
        for n in range(2):
            tile = 2 * turn + n
            gather_markers(
                tile, zero, live_tiles, index_s, table, across.at[tile], along.at[tile], depth.at[tile], stages[n], velocity
            )

    for k in range(GROUPS):
        new_copy(k, *span(k)).wait()


def gather(count, offsets, base_x, base_y, base_z, u_old, density, grid, *received):
    return pl.pallas_call(
        gather_kernel,
        name="gather",
        in_specs=[pl.BlockSpec(memory_space=SMEM)]
        + [pl.BlockSpec(memory_space=VMEM)] * 4
        + [pl.BlockSpec(memory_space=HBM)] * (3 + len(EXCHANGED)),
        out_specs=[pl.BlockSpec(memory_space=HBM), pl.BlockSpec(memory_space=VMEM)],
        out_shape=[
            jax.ShapeDtypeStruct((3, SIDE, SIDE, NZ), F32),
            jax.ShapeDtypeStruct((3, SLOTS, LANES), F32),
        ],
        scratch_shapes=[
            VMEM((SLOTS, LANES), I32),
            SMEM((SLOTS, LANES), I32),
            VMEM((ROWS, LANES), F32),
            VMEM((4, PLANES, SIDE, NZ), F32),
            VMEM((PLANES, 3, 2, 40, LANES), F32),
        ]
        + [VMEM(shape, F32) for shape in EXCHANGED[:5]]
        + [VMEM(EXCHANGED[1], F32)]
        + [
            VMEM((SLOTS, 4, LANES, LANES), F32),
            VMEM((SLOTS, 4, LANES, LANES), F32),
            VMEM((SLOTS, 3, LANES, LANES), F32),
            VMEM((4 * LANES, LANES), F32),
            VMEM((4 * LANES, LANES), F32),
            pltpu.SemaphoreType.DMA((10,)),
            pltpu.SemaphoreType.DMA((7,)),
            pltpu.SemaphoreType.DMA((2, GROUPS)),
            pltpu.SemaphoreType.DMA((GROUPS,)),
        ],
        compiler_params=pltpu.CompilerParams(vmem_limit_bytes=63 * 2**20),
    )(count, offsets, base_x, base_y, base_z, u_old, density, grid, *received)


def on_device(u_old, density, offsets, forces, base_x, base_y, base_z, tile_count):
    grid, strip, low, high, side = spread(tile_count, offsets, forces, base_x, base_y, base_z, u_old, density)
    received = exchange(side, strip, low, high, density)
    return tuple(gather(tile_count, offsets, base_x, base_y, base_z, u_old, density, grid, *received))


def solution(mesh):
    tiles = P(("gx", "gy"), None)
    in_specs = (
        P(None, "gx", "gy", None),
        P("gx", "gy", None),
        P(None, ("gx", "gy"), None),
        P(None, ("gx", "gy"), None),
        tiles,
        tiles,
        tiles,
        P(("gx", "gy")),
    )
    out_specs = (P(None, "gx", "gy", None), P(None, ("gx", "gy"), None))
    return jax.shard_map(on_device, mesh=mesh, in_specs=in_specs, out_specs=out_specs, check_vma=False)
```

```python
import functools

import jax
import jax.numpy as jnp
from jax import lax
from jax.experimental import pallas as pl
from jax.experimental.pallas import tpu as pltpu
from jax.sharding import PartitionSpec as P

F32 = jnp.float32
I32 = jnp.int32
HBM = pltpu.HBM
VMEM = pltpu.VMEM
SMEM = pltpu.SMEM

SLOTS = 16
LANES = 128
SIDE = 32
NZ = 256
NT = 7
ZS, ZW = 37, 40
CS = 42
PLANES = 35
GROUPS = 7
BLOCK = 40
STEP = NT * BLOCK
FRONT = 8
ROWS = 9856
COPIES = 2
EARLY = 368
PART = 32


def iota(shape, dim):
    return lax.broadcasted_iota(I32, shape, dim)


def four_weights(frac, root):
    low, high = 3.0 - 2.0 * frac, 1.0 + 2.0 * frac
    return [(low - root) * 0.125, (low + root) * 0.125, (high + root) * 0.125, (high - root) * 0.125]


def root_of(frac):
    return jnp.sqrt(1.0 + 4.0 * frac - 4.0 * frac * frac)


def row_index(bx, by, bz):
    z_tile = lax.shift_right_logical(bz * 1772, 16)
    return (bx * NT + z_tile) * BLOCK + by + FRONT


def columns_of(rows):
    rows = rows + [rows[-1]] * (-len(rows) % 8)
    return jnp.concatenate(rows, axis=0).T


def depth_weights(place, frac, root):
    away = iota((8, LANES), 1).astype(F32) - place
    away = jnp.where(away < 0.0, away + 128.0, away)
    first, second = away < CS - 0.5, away < 2 * CS - 0.5
    k = away - jnp.where(first, 0.0, jnp.where(second, float(CS), float(2 * CS)))
    value = jnp.where(k < 1.5, 3.0 - 2.0 * frac, 1.0 + 2.0 * frac)
    value = (value + jnp.where(jnp.abs(k - 1.5) < 1.0, root, -root)) * 0.125
    value = jnp.where(k < 3.5, value, 0.0)
    later = jnp.where(first, 0.0, value)
    return [jnp.where(first, value, 0.0), jnp.where(second, later, 0.0), jnp.where(second, 0.0, later)]


def z_place(bz):
    return lax.bitwise_and(bz + 127, 127).astype(F32)


def segments(t):
    found = []
    for half in range(2):
        for turn in (-1, 0, 1):
            low = max(ZS * t - 1 + NZ * turn - LANES * half, 0)
            high = min(ZS * t - 1 + ZW + NZ * turn - LANES * half, LANES)
            if low < high:
                found.append((half, low, high))
    return found


def lane_mask(c, low, high):
    lane = lax.bitwise_and(iota((8, LANES), 1) + (LANES - CS * c), 127)
    if low == 0:
        return lane < high
    if high == LANES:
        return lane >= low
    return jnp.logical_and(lane >= low, lane < high)


def spread_columns(tile, count, offsets, forces, base_z):
    live = jnp.where(tile < count, 1.0, 0.0)
    sy, sz = (offsets[i, pl.ds(tile, 1), :] for i in (1, 2))
    push = [forces[c, pl.ds(tile, 1), :] * live for c in range(3)]
    return columns_of([z_place(base_z[pl.ds(tile, 1), :]), sz, root_of(sz)] + push + [sy, root_of(sy)])


def spread_wide(tables, tile, g):
    rows = tables[jnp.minimum(tile, SLOTS - 1), pl.ds(pl.multiple_of(8 * g, 8), 8), :]
    return [jnp.broadcast_to(rows[:, n : n + 1], (8, LANES)) for n in range(8)]


def spread_store(wide, g, line):
    depth = sum(w * part for w, part in zip(wide[3:6], depth_weights(*wide[:3])))
    for b, weight in enumerate(four_weights(wide[6], wide[7])):
        line[pl.ds(g * 32 + b, 8, stride=4), :] = weight * depth


def spread_group(tile, part, zero, first, index_s, across_s, line, grids):
    made = []
    for n in range(COPIES):
        m = first + n
        start = index_s[part, tile, m]
        rows = line[pl.ds(zero + m * 4, 4), :]
        for a in range(4):
            where = pl.ds(start + a * STEP, 4)
            made.append((grids[n], where, grids[n][where, :] + across_s[part, tile, PART * a + m] * rows))
    for grid, where, value in made:
        grid[where, :] = value


def spread_kernel(
    count, offsets, forces, base_x, base_y, base_z, u_old, density,
    grid_out, strip_out, low_out, high_out, side_out,
    *scratch,
):
    grids = scratch[:COPIES]
    (index_v, index_s, across_v, across_s, tables, line_a, line_b, planes, strips, edge_low, edge_high, low_v, high_v,
     side_u, side_v, sems, plane_sems) = scratch[COPIES:]
    index = row_index(base_x[...], base_y[...], base_z[...])
    for part in range(LANES // PART):
        index_v[part] = pltpu.roll(index, LANES - PART * part, 1) if part else index
    weights = four_weights(offsets[0], root_of(offsets[0]))
    lane = iota((SLOTS, LANES), 1)
    for part in range(LANES // PART):
        total = None
        for a in range(4):
            moved = pltpu.roll(weights[a], PART * (a - part) % LANES, 1) if a != part else weights[a]
            total = moved if total is None else jnp.where(lane >= PART * a, moved, total)
        across_v[part] = total
    to_smem = pltpu.make_async_copy(index_v, index_s, sems.at[0])
    to_smem.start()
    across_copy = pltpu.make_async_copy(across_v, across_s, sems.at[9])
    across_copy.start()
    inner, uvw = pl.ds(1, SIDE), pl.ds(0, 3)
    edges = []
    for first, place in ((0, edge_low), (SIDE - 8, edge_high)):
        edges.append((u_old.at[:, :, pl.ds(first, 8), :], place.at[uvw, inner]))
        edges.append((density.at[:, pl.ds(first, 8), :], place.at[3, inner]))
    for first, size, at in ((0, 2, 0), (SIDE - 1, 1, 2)):
        edges.append((u_old.at[:, pl.ds(first, size)], side_u.at[uvw, pl.ds(at, size)]))
        edges.append((density.at[pl.ds(first, size)], side_u.at[3, pl.ds(at, size)]))
    edges = [pltpu.make_async_copy(source, target, sems.at[1 + n]) for n, (source, target) in enumerate(edges)]
    for copy in edges:
        copy.start()

    live_tiles = count[0]
    columns = functools.partial(spread_columns, count=live_tiles, offsets=offsets, forces=forces, base_z=base_z)
    nothing = jnp.zeros((8, LANES), F32)
    for tile in range(SLOTS):
        tables[tile] = columns(tile)
        for i in range(tile * EARLY // SLOTS, (tile + 1) * EARLY // SLOTS):
            for grid in grids:
                grid[8 * i : 8 * i + 8, :] = nothing
    for g in range(LANES // 8):
        spread_store(spread_wide(tables, 0, g), g, line_a)

    @pl.loop(EARLY // 16, ROWS // 128)
    def _(i):
        for grid in grids:
            for j in range(16):
                grid[pl.ds(i * 128 + j * 8, 8), :] = nothing

    to_smem.wait()
    across_copy.wait()

    @pl.loop(0, lax.shift_right_logical(live_tiles + 1, 1))
    def _(turn):
        for n, (now, later) in enumerate(((line_a, line_b), (line_b, line_a))):
            tile = 2 * turn + n

            @pl.loop(0, LANES // PART)
            def _(part):
                chunks = [part * (PART // 8) + j for j in range(PART // 8)]
                wide = [spread_wide(tables, tile + 1, g) for g in chunks]
                line = now.at[pl.ds(pl.multiple_of(part * 4 * PART, 8), 4 * PART), :]
                for first in range(0, PART, COPIES):
                    spread_group(tile, part, jnp.minimum(part, 0), first, index_s, across_s, line, grids)
                for g, values in zip(chunks, wide):
                    spread_store(values, g, later)

    for copy in edges:
        copy.wait()
    row = iota((8, LANES), 0)
    three_rows = row < 3
    own_rows = (jnp.logical_or(row == 1, row == 2), row == 0)

    @pl.loop(0, SIDE)
    def _(x):
        for half in range(2):
            lanes = slice(half * LANES, (half + 1) * LANES)
            low_v[half, pl.ds(x * 2, 8), :] = edge_low[3, x + 1, :, lanes]
            high_v[half, pl.ds(x, 8), :] = pltpu.roll(edge_high[3, x + 1, :, lanes], 1, 0)

    def plane_copy(k):
        return pltpu.make_async_copy(planes.at[pl.ds(5 * k, 5)], grid_out.at[pl.ds(5 * k, 5)], plane_sems.at[k])

    @pl.loop(0, PLANES // 5)
    def _(k):
        for i in range(5):
            x = 5 * k + i
            ours = jnp.logical_and(x > 0, x <= SIDE)
            for yb in range(5):
                if yb in (0, 4):
                    edge = edge_high if yb else edge_low
                    halves = (slice(0, LANES), slice(LANES, 2 * LANES))
                    rate = [0.5 / pltpu.roll(edge[3, x, :, lanes], 1, 0) for lanes in halves]
                tiles = []
                for t in range(NT):
                    start = pl.multiple_of(FRONT + (x * NT + t) * BLOCK, 8) + 8 * yb
                    tiles.append(sum(grid[pl.ds(pl.multiple_of(start, 8), 8), :] for grid in grids))
                for c in range(3):
                    for half in range(2):
                        total = None
                        for group in ((0, 2, 4), (1, 3, 5), (6,)):
                            part = None
                            for t in group:
                                for at, low, high in segments(t):
                                    if at == half:
                                        part = jnp.where(lane_mask(c, low, high), tiles[t], 0.0 if part is None else part)
                            if part is not None:
                                total = part if total is None else total + part
                        if c:
                            total = pltpu.roll(total, LANES - CS * c, 1)
                        planes[x, c, half, 8 * yb : 8 * yb + 8, :] = total
                        if yb in (0, 4):
                            known = pltpu.roll(edge[c, x, :, halves[half]], 1, 0) + total * rate[half]
                            value = jnp.where(jnp.logical_and(own_rows[yb // 4], ours), known, total)
                            strips[yb // 4, half, pl.ds((x * 3 + c) * 3, 8), :] = jnp.where(three_rows, value, 0.0)

        plane_copy(k).start()

    last_row, first_row = row == 7, row == 0
    for n, (side, at, plane) in enumerate(((0, 1, 0), (0, 2, 1), (1, 0, 2))):
        x = SIDE * side + at

        @pl.loop(0, 2)
        def _(half):
            lanes = pl.ds(pl.multiple_of(half * LANES, LANES), LANES)

            def shifted_rows(c, yb):
                here = side_u[c, plane, 8 * min(yb, 3) : 8 * min(yb, 3) + 8, lanes]
                before = side_u[c, plane, 8 * max(yb - 1, 0) : 8 * max(yb - 1, 0) + 8, lanes]
                return pltpu.roll(jnp.where(last_row, before, here), 1, 0)

            for yb in range(5):
                rows = slice(8 * yb, 8 * yb + 8)
                size = min(8, PLANES - 8 * yb)
                rate = 0.5 / shifted_rows(3, yb)
                for c in range(3):
                    force = planes[x, c, half, rows, :]
                    value = shifted_rows(c, yb) + force * rate
                    if yb == 0:
                        value = jnp.where(first_row, force, value)
                    if yb == 4:
                        value = jnp.where(first_row, value, force)
                    side_v[side, pl.ds(((at * 3 + c) * 2 + half) * PLANES + 8 * yb, size), :] = value[:size]

    for side, at in ((0, 0), (1, 1), (1, 2)):

        @pl.loop(0, 3)
        def _(c):
            for half in range(2):
                for yb in range(5):
                    size = min(8, PLANES - 8 * yb)
                    value = planes[SIDE * side + at, c, half, 8 * yb : 8 * yb + 8, :]
                    side_v[side, pl.ds(((at * 3 + c) * 2 + half) * PLANES + 8 * yb, size), :] = value[:size]

    tail = [
        pltpu.make_async_copy(strips, strip_out, sems.at[0]),
        pltpu.make_async_copy(low_v, low_out, sems.at[1]),
        pltpu.make_async_copy(high_v, high_out, sems.at[2]),
        pltpu.make_async_copy(side_v, side_out, sems.at[3]),
    ]
    for copy in tail:
        copy.start()
    for copy in tail:
        copy.wait()
    for k in range(PLANES // 5):
        plane_copy(k).wait()


LOW_ROWS = 72
HIGH_ROWS = 40
YROWS = 320
SIDE_ROWS = 640


def spread(count, offsets, forces, base_x, base_y, base_z, u_old, density):
    return pl.pallas_call(
        spread_kernel,
        name="spread",
        in_specs=[pl.BlockSpec(memory_space=SMEM)] + [pl.BlockSpec(memory_space=VMEM)] * 5 + [pl.BlockSpec(memory_space=HBM)] * 2,
        out_specs=[pl.BlockSpec(memory_space=HBM)] * 5,
        out_shape=[
            jax.ShapeDtypeStruct((PLANES, 3, 2, 40, LANES), F32),
            jax.ShapeDtypeStruct((2, 2, YROWS, LANES), F32),
            jax.ShapeDtypeStruct((2, LOW_ROWS, LANES), F32),
            jax.ShapeDtypeStruct((2, HIGH_ROWS, LANES), F32),
            jax.ShapeDtypeStruct((2, SIDE_ROWS, LANES), F32),
        ],
        scratch_shapes=[VMEM((ROWS, LANES), F32)] * COPIES
        + [VMEM((LANES // PART, SLOTS, LANES), I32), SMEM((LANES // PART, SLOTS, LANES), I32)]
        + [VMEM((LANES // PART, SLOTS, LANES), F32), SMEM((LANES // PART, SLOTS, LANES), F32)]
        + [VMEM((SLOTS, LANES, 8), F32)]
        + [VMEM((4 * LANES, LANES), F32)] * 2
        + [
            VMEM((PLANES, 3, 2, 40, LANES), F32),
            VMEM((2, 2, YROWS, LANES), F32),
            VMEM((4, PLANES, 8, NZ), F32),
            VMEM((4, PLANES, 8, NZ), F32),
            VMEM((2, LOW_ROWS, LANES), F32),
            VMEM((2, HIGH_ROWS, LANES), F32),
            VMEM((4, 3, SIDE, NZ), F32),
            VMEM((2, SIDE_ROWS, LANES), F32),
            pltpu.SemaphoreType.DMA((10,)),
            pltpu.SemaphoreType.DMA((PLANES // 5,)),
        ],
        compiler_params=pltpu.CompilerParams(vmem_limit_bytes=63 * 2**20),
    )(count, offsets, forces, base_x, base_y, base_z, u_old, density)


def exchange_kernel(
    side, strip, low, high, density,
    rx, ry, rd, rlow, rhigh, dx_low, dx_high,
    send_sems, recv_sems,
):
    nx, ny = lax.axis_size("gx"), lax.axis_size("gy")
    gx, gy = lax.axis_index("gx"), lax.axis_index("gy")
    left, right = lax.rem(gx + nx - 1, nx), lax.rem(gx + 1, nx)
    down, up = lax.rem(gy + ny - 1, ny), lax.rem(gy + 1, ny)
    around = [(i, j) for i in (left, gx, right) for j in (down, gy, up)]
    del around[4]
    barrier = pltpu.get_barrier_semaphore()
    for place in around:
        pl.semaphore_signal(barrier, inc=1, device_id=place, device_id_type=pl.DeviceIdType.MESH)
    pl.semaphore_wait(barrier, len(around))
    last = pl.ds(SIDE - 1, 1)
    first = pl.ds(0, 2)
    rows = lambda start, size: pl.ds(start, size)
    moves = [
        (strip.at[1, :, rows(0, 320), :], ry.at[0], (gx, up)),
        (strip.at[0, :, rows(0, 320), :], ry.at[1], (gx, down)),
        (low.at[:, rows(0, 64), :], rlow.at[:, rows(8, 64), :], (gx, down)),
        (high.at[:, rows(0, 32), :], rhigh.at[:, rows(8, 32), :], (gx, up)),
        (side.at[1], rx.at[0], (right, gy)),
        (side.at[0], rx.at[1], (left, gy)),
        (density.at[last], dx_low, (right, gy)),
        (density.at[first], dx_high, (left, gy)),
        (strip.at[1, :, rows(288, 32), :], rd.at[0], (right, up)),
        (high.at[:, rows(24, 8), :], rhigh.at[:, rows(0, 8), :], (right, up)),
        (strip.at[1, :, rows(0, 32), :], rd.at[1], (left, up)),
        (high.at[:, rows(0, 8), :], rhigh.at[:, rows(40, 8), :], (left, up)),
        (strip.at[0, :, rows(288, 32), :], rd.at[2], (right, down)),
        (low.at[:, rows(56, 8), :], rlow.at[:, rows(0, 8), :], (right, down)),
        (strip.at[0, :, rows(0, 32), :], rd.at[3], (left, down)),
        (low.at[:, rows(0, 8), :], rlow.at[:, rows(72, 8), :], (left, down)),
    ]
    copies = [
        pltpu.make_async_remote_copy(
            src_ref=source,
            dst_ref=target,
            send_sem=send_sems.at[n],
            recv_sem=recv_sems.at[n],
            device_id=place,
            device_id_type=pl.DeviceIdType.MESH,
        )
        for n, (source, target, place) in enumerate(moves)
    ]
    for copy in copies:
        copy.start()
    for copy in copies:
        copy.wait()


MOVES = 16
RLOW_ROWS, RHIGH_ROWS = 88, 56
EXCHANGED = (
    (2, SIDE_ROWS, LANES),
    (2, 2, 320, LANES),
    (4, 2, 32, LANES),
    (2, RLOW_ROWS, LANES),
    (2, RHIGH_ROWS, LANES),
    (1, SIDE, NZ),
    (2, SIDE, NZ),
)


def exchange(side, strip, low, high, density):
    return pl.pallas_call(
        exchange_kernel,
        name="exchange",
        in_specs=[pl.BlockSpec(memory_space=HBM)] * 5,
        out_specs=[pl.BlockSpec(memory_space=HBM)] * len(EXCHANGED),
        out_shape=[jax.ShapeDtypeStruct(shape, F32) for shape in EXCHANGED],
        scratch_shapes=[pltpu.SemaphoreType.DMA((MOVES,)), pltpu.SemaphoreType.DMA((MOVES,))],
        compiler_params=pltpu.CompilerParams(collective_id=0, has_side_effects=True),
    )(side, strip, low, high, density)


def gather_build(tile, offsets, base_z, across, along, depth):
    sx, sy, sz = (offsets[i, pl.ds(tile, 1), :] for i in range(3))
    table = columns_of([z_place(base_z[pl.ds(tile, 1), :]), sz, root_of(sz), sy, root_of(sy), sx, root_of(sx)])
    for g in range(LANES // 8):
        rows = slice(8 * g, 8 * g + 8)
        wide = [jnp.broadcast_to(table[rows, n : n + 1], (8, LANES)) for n in range(7)]
        for c, value in enumerate(depth_weights(wide[0], wide[1], wide[2])):
            depth[c, rows, :] = value
        for b, weight in enumerate(four_weights(wide[3], wide[4])):
            along[b, rows, :] = weight
        for a, weight in enumerate(four_weights(wide[5], wide[6])):
            across[a, rows, :] = weight


def gather_markers(tile, zero, count, index_s, table, across, along, depth, stage, velocity):
    for m in range(LANES):
        start = index_s[tile, m]
        total = None
        for a in range(4):
            term = jnp.broadcast_to(across[a, m : m + 1, :], (4, LANES)) * table[pl.ds(start + a * STEP, 4), :]
            total = term if total is None else total + term
        stage[pl.ds(zero + m * 4, 4), :] = total
    picked = [[] for _ in range(3)]
    for g in range(LANES // 8):
        rows = slice(8 * g, 8 * g + 8)
        total = None
        for b in range(4):
            term = along[b, rows, :] * stage[pl.ds(zero + g * 32 + b, 8, stride=4), :]
            total = term if total is None else total + term
        for c in range(3):
            picked[c].append(total * depth[c, rows, :])
    values = jnp.concatenate(picked[0] + picked[1] + picked[2], axis=0)
    rough = values.astype(jnp.bfloat16)
    rest = (values - rough.astype(F32)).astype(jnp.bfloat16)
    both = jnp.concatenate([rough, rest], axis=1)
    out = lax.dot_general(
        jnp.ones((8, 2 * LANES), jnp.bfloat16), both, (((1,), (1,)), ((), ())), preferred_element_type=F32
    )
    for c in range(3):
        velocity[c, pl.ds(tile, 1), :] = jnp.where(tile < count, out[0:1, c * LANES : (c + 1) * LANES], 0.0)


def gather_kernel(
    count, offsets, base_x, base_y, base_z, u_old, density, grid,
    rx, ry, rd, rlow, rhigh, dx_low, dx_high,
    u_new, velocity,
    index_v, index_s, table, fluid, force, vx, vy, vd, vlow, vhigh, corner,
    across, along, depth, stage_a, stage_b, sems, force_sems, old_sems, new_sems,
):
    inner = pl.ds(0, SIDE)
    uvw = pl.ds(0, 3)
    loads = [
        (rx, vx),
        (ry, vy),
        (rd, vd),
        (rlow, vlow),
        (rhigh, vhigh),
        (dx_low, fluid.at[3, pl.ds(0, 1), inner, :]),
        (dx_high, fluid.at[3, pl.ds(SIDE + 1, 2), inner, :]),
    ]
    copies = [pltpu.make_async_copy(source, target, sems.at[1 + n]) for n, (source, target) in enumerate(loads)]
    for copy in copies:
        copy.start()

    def force_copy(k):
        return pltpu.make_async_copy(grid.at[pl.ds(5 * k, 5)], force.at[pl.ds(5 * k, 5)], force_sems.at[k])

    def old_copies(k, first, size):
        here, there = pl.ds(first, size), pl.ds(first + 1, size)
        return (
            pltpu.make_async_copy(u_old.at[:, here], fluid.at[uvw, there, inner, :], old_sems.at[0, k]),
            pltpu.make_async_copy(density.at[here], fluid.at[3, there, inner, :], old_sems.at[1, k]),
        )

    def new_copy(k, first, size):
        return pltpu.make_async_copy(
            fluid.at[uvw, pl.ds(first + 1, size), inner, :], u_new.at[:, pl.ds(first, size)], new_sems.at[k]
        )

    def span(k):
        first, last = max(5 * k - 1, 0), min(5 * k + 4, SIDE)
        return first, last - first

    def each_span(k, act):
        pl.when(k == 0)(lambda: act(k, *span(0)))
        pl.when(k == GROUPS - 1)(lambda: act(k, *span(GROUPS - 1)))
        pl.when(jnp.logical_and(k > 0, k < GROUPS - 1))(lambda: act(k, 5 * k - 1, 5))

    def wait_old(*where):
        for copy in old_copies(*where):
            copy.wait()

    def start_new(*where):
        new_copy(*where).start()

    stages = (stage_a, stage_b)
    for k in range(GROUPS):
        force_copy(k).start()
        for copy in old_copies(k, *span(k)):
            copy.start()
    index_v[...] = row_index(base_x[...], base_y[...], base_z[...])
    to_smem = pltpu.make_async_copy(index_v, index_s, sems.at[0])
    to_smem.start()
    velocity[...] = jnp.zeros_like(velocity)
    live_tiles = count[0]

    pairs = lax.shift_right_logical(live_tiles + 1, 1)

    @pl.loop(0, pairs)
    def _(turn):
        for tile in (2 * turn, 2 * turn + 1):
            gather_build(tile, offsets, base_z, across.at[tile], along.at[tile], depth.at[tile])

    to_smem.wait()
    for copy in copies:
        copy.wait()
    corner[...] = jnp.zeros_like(corner)
    for n in range(4):
        right, down = n % 2, n // 2
        for half in range(2):
            corner[down, half, pl.ds(288 * right, 32), :] = vd[n, half]

    row = iota((8, LANES), 0)
    first_row, last_row = row == 0, row == 7
    two_rows = row < 2
    inside = jnp.logical_or(last_row, two_rows)

    def plane(x, zero):
        halo = jnp.logical_or(x == 0, x > SIDE)
        fresh = [[[None, None] for _ in range(3)] for _ in range(5)]
        for half in range(2):
            lanes = slice(half * LANES, (half + 1) * LANES)

            edge = jnp.where(last_row, vhigh[half, pl.ds(x, 8), :], vlow[half, pl.ds(x * 2 + 6, 8), :])
            rate = [0.5 / fluid[3, x, 8 * yb : 8 * yb + 8, lanes] for yb in range(4)] + [0.5 / jnp.where(inside, edge, 1.0)]
            for c in range(3):
                push = [force[x, c, half, pl.ds(zero + 8 * yb + 1, 8), :] for yb in range(4)]
                where = pl.ds((x * 3 + c) * 3, 8)
                below, above = (pltpu.roll(vy[n, half, where, :], 7, 0) for n in range(2))
                far_below, far_above = (pltpu.roll(corner[n, half, where, :], 7, 0) for n in range(2))
                push[0] = push[0] + jnp.where(two_rows, below + far_below, 0.0)
                push[3] = push[3] + jnp.where(last_row, above + far_above, 0.0)
                for yb in range(4):
                    value = fluid[c, x, 8 * yb : 8 * yb + 8, lanes] + push[yb] * rate[yb]
                    fluid[c, x, 8 * yb : 8 * yb + 8, lanes] = value
                    fresh[yb][c][half] = value
                outer = pltpu.roll(jnp.where(first_row, force[x, c, half, 0:8, :], force[x, c, half, 32:40, :]), 7, 0)
                near, far = jnp.where(last_row, below, above), jnp.where(last_row, far_below, far_above)
                known, other = jnp.where(halo, far, near), jnp.where(halo, near, far)
                fresh[4][c][half] = jnp.where(inside, known + (outer + other) * rate[4], 0.0)
        packed = []
        for yb in range(5):
            moved = [[pltpu.roll(v, CS * c, 1) if c else v for v in fresh[yb][c]] for c in range(3)]
            tiles = []
            for t in range(NT):
                value = None
                for c in range(3):
                    for half, low, high in segments(t):
                        piece = moved[c][half]
                        value = piece if value is None else jnp.where(lane_mask(c, low, high), piece, value)
                tiles.append(value)
            packed.append(tiles)
        for t in range(NT):
            start = FRONT + (x * NT + t) * BLOCK
            table[pl.ds(start, 8), :] = pltpu.roll(packed[4][t], 1, 0)
            for yb in range(5):
                table[pl.ds(start + 8 * yb + 1, 8), :] = packed[yb][t]

    @pl.loop(0, GROUPS)
    def _(k):
        force_copy(k).wait()
        each_span(k, wait_old)

        def take_side(side, n):
            x = SIDE * side + n
            other = (side, n) not in ((0, 1), (0, 2), (1, 0))

            @pl.loop(0, 3)
            def _(c):
                for half in range(2):
                    lanes = slice(half * LANES, (half + 1) * LANES)
                    start = ((n * 3 + c) * 2 + half) * PLANES
                    value = [vx[side, pl.ds(start + 8 * yb, 8), :] for yb in range(5)]
                    if other:
                        for yb in range(4):
                            fluid[c, x, 8 * yb : 8 * yb + 8, lanes] = vx[side, pl.ds(start + 8 * yb + 1, 8), :]
                        value = [jnp.where(first_row, value[0], 0.0), None, None, None, jnp.where(first_row, 0.0, value[4])]
                    for yb in range(5):
                        if value[yb] is not None:
                            force[x, c, half, 8 * yb : 8 * yb + 8, :] += value[yb]

        @pl.when(k == 0)
        def _():
            for n in range(3):
                take_side(0, n)

        @pl.when(k == GROUPS - 1)
        def _():
            for n in range(3):
                take_side(1, n)

        zero = jnp.minimum(k, 0)
        for i in range(5):
            plane(5 * k + i, zero)
        each_span(k, start_new)

    @pl.loop(0, pairs)
    def _(turn):
        zero = jnp.minimum(turn, 0)
        for n in range(2):
            tile = 2 * turn + n
            gather_markers(
                tile, zero, live_tiles, index_s, table, across.at[tile], along.at[tile], depth.at[tile], stages[n], velocity
            )

    for k in range(GROUPS):
        new_copy(k, *span(k)).wait()


def gather(count, offsets, base_x, base_y, base_z, u_old, density, grid, *received):
    return pl.pallas_call(
        gather_kernel,
        name="gather",
        in_specs=[pl.BlockSpec(memory_space=SMEM)]
        + [pl.BlockSpec(memory_space=VMEM)] * 4
        + [pl.BlockSpec(memory_space=HBM)] * (3 + len(EXCHANGED)),
        out_specs=[pl.BlockSpec(memory_space=HBM), pl.BlockSpec(memory_space=VMEM)],
        out_shape=[
            jax.ShapeDtypeStruct((3, SIDE, SIDE, NZ), F32),
            jax.ShapeDtypeStruct((3, SLOTS, LANES), F32),
        ],
        scratch_shapes=[
            VMEM((SLOTS, LANES), I32),
            SMEM((SLOTS, LANES), I32),
            VMEM((ROWS, LANES), F32),
            VMEM((4, PLANES, SIDE, NZ), F32),
            VMEM((PLANES, 3, 2, 40, LANES), F32),
        ]
        + [VMEM(shape, F32) for shape in EXCHANGED[:5]]
        + [VMEM(EXCHANGED[1], F32)]
        + [
            VMEM((SLOTS, 4, LANES, LANES), F32),
            VMEM((SLOTS, 4, LANES, LANES), F32),
            VMEM((SLOTS, 3, LANES, LANES), F32),
            VMEM((4 * LANES, LANES), F32),
            VMEM((4 * LANES, LANES), F32),
            pltpu.SemaphoreType.DMA((10,)),
            pltpu.SemaphoreType.DMA((7,)),
            pltpu.SemaphoreType.DMA((2, GROUPS)),
            pltpu.SemaphoreType.DMA((GROUPS,)),
        ],
        compiler_params=pltpu.CompilerParams(vmem_limit_bytes=63 * 2**20),
    )(count, offsets, base_x, base_y, base_z, u_old, density, grid, *received)


def on_device(u_old, density, offsets, forces, base_x, base_y, base_z, tile_count):
    grid, strip, low, high, side = spread(tile_count, offsets, forces, base_x, base_y, base_z, u_old, density)
    received = exchange(side, strip, low, high, density)
    return tuple(gather(tile_count, offsets, base_x, base_y, base_z, u_old, density, grid, *received))


def solution(mesh):
    tiles = P(("gx", "gy"), None)
    in_specs = (
        P(None, "gx", "gy", None),
        P("gx", "gy", None),
        P(None, ("gx", "gy"), None),
        P(None, ("gx", "gy"), None),
        tiles,
        tiles,
        tiles,
        P(("gx", "gy")),
    )
    out_specs = (P(None, "gx", "gy", None), P(None, ("gx", "gy"), None))
    return jax.shard_map(on_device, mesh=mesh, in_specs=in_specs, out_specs=out_specs, check_vma=False)
```
